32 devices in a mesh: ctx: 16 (over z, x, core), head: 1, tp: 2 (over y).
Axes of the slice: x: 2, y: 2, z: 4, core: 2. Of those that a mesh axis runs over, the one named last changes fastest.
Arguments:
- text_states: bfloat16 [256, 8192], P(None, 'ctx'), may hold values from -6 to 6
- q_weight: bfloat16 [8192, 8192], P('ctx', ('head', 'tp')), may hold values from -0.0625 to 0.0625
- q_gain: float32 [128], replicated, may hold values from 0.1 to 1.9
- visual_key_cache: bfloat16 [8192, 1024], P('ctx', ('head', 'tp')), may hold values from -400 to 400
- visual_value_cache: bfloat16 [8192, 1024], P('ctx', ('head', 'tp')), may hold values from -6 to 6
- block_mask: int32 [256, 32], P(None, 'ctx'), may hold values from 0 to 1, as said below
- lengths: int32 [256], replicated, may hold values from 256 to 8192, as said below
- o_weight: bfloat16 [8192, 8192], P(('head', 'tp'), 'ctx'), may hold values from -0.59765625 to 0.59765625
Outputs:
- updated: bfloat16 [256, 8192], P(('head', 'tp'), 'ctx')
The draws below stay inside these ranges and needn't reach their ends.
Inputs may be any that keep to these rules, and one draw needn't show every extreme that they name: `block_mask`: segment 0 is visible to every row. `lengths`: some row sees all 8192 tokens.
All inputs are finite; a program needn't handle non-finite values.
Results may differ from the reference program's by a relative error of at most 0.0055.
Values may be sent and summed in bfloat16 or wider, within the bound.
No kernel may reach another device: no remote copies, remote signals or barrier semaphores. Data moves between devices by JAX's collectives and lax.ppermute only.
A program may use at most 64 MiB of HBM per device.

```python
import jax
import jax.numpy as jnp
from jax import lax

D = 8192
QUERY_HEAD_COUNT = 64
KEY_VALUE_HEADS = 8
HEAD_SIZE = 128
TEXT = 256
VISUAL_PER_CTX = 512
SEG = 256
VISUAL_TOKENS = 8192
NSEG = 32
N_CTX = 16


def draw_visual_key_cache(key, part):
    initial_random_key = jax.random.fold_in(key, 11)
    random_base_seed = 2.0 * jax.random.truncated_normal(initial_random_key, -4.0, 4.0, (VISUAL_TOKENS, KEY_VALUE_HEADS * HEAD_SIZE), jnp.float32)
    result = random_base_seed
    return result.astype(jnp.bfloat16)


def draw_block_mask(key, part):
    initial_random_key = jax.random.fold_in(key, 21)
    visible = jax.random.randint(initial_random_key, (TEXT, NSEG), 0, 2).astype(jnp.int32)
    return visible.at[:, 0].set(1)


def draw_lengths(key, part):
    initial_random_key = jax.random.fold_in(key, 31)
    second_key = jax.random.fold_in(key, 32)
    drawn = jax.random.randint(initial_random_key, (TEXT,), SEG, VISUAL_TOKENS + 1).astype(jnp.int32)
    chosen = jax.random.randint(second_key, (), 0, TEXT)
    return drawn.at[chosen].set(VISUAL_TOKENS)


def shard_levels(key, shape, split, low, largest):
    factor_of, own = 1.0, jax.random.fold_in(key, 6)
    for dim, parts in split:
        heights = jnp.exp(jax.random.uniform(jax.random.fold_in(own, dim), (parts,), jnp.float32, low / len(split), largest / len(split)))
        factor_of = factor_of * jnp.repeat(heights, shape[dim] // parts).reshape([-1 if axis == dim else 1 for axis in range(len(shape))])
    return factor_of


def gaussian(rng, shape, width, reach, pieces=(), kind=jnp.bfloat16):
    values = jax.random.normal(rng, shape, jnp.float32) * width
    if len(pieces) > 0:
        values = shard_levels(rng, shape, pieces, -0.22, 0.18) * values
    return jnp.clip(values, min=-reach, max=reach).astype(kind)


def setup_inputs(seed: int = 0) -> dict:
    keys = jax.random.split(jax.random.key(seed), 9)
    return {
        "text_states": gaussian(keys[0], (TEXT, D), 1.0, 6.0, ((1, 16),)),
        "q_weight": gaussian(keys[1], (D, QUERY_HEAD_COUNT * HEAD_SIZE), D ** -0.5, 0.0625, ((0, 16), (1, 2))),
        "q_gain": jnp.clip(1.0 + 0.18 * jax.random.normal(keys[2], (HEAD_SIZE,), jnp.float32), 0.1, 1.9),
        "visual_key_cache": draw_visual_key_cache(jax.random.fold_in(keys[8], 71), 0),
        "visual_value_cache": gaussian(keys[4], (VISUAL_TOKENS, KEY_VALUE_HEADS * HEAD_SIZE), 1.0, 6.0, ((0, 16), (1, 2))),
        "block_mask": draw_block_mask(jax.random.fold_in(keys[8], 71), 0),
        "lengths": draw_lengths(jax.random.fold_in(keys[8], 71), 0),
        "o_weight": gaussian(keys[7], (QUERY_HEAD_COUNT * HEAD_SIZE, D), 0.1, 0.59765625, ((0, 2), (1, 16))),
    }


def reference(text_states, q_weight, q_gain, visual_key_cache, visual_value_cache, block_mask, lengths, o_weight):
    queries = jnp.dot(text_states, q_weight, preferred_element_type=jnp.float32)
    shaped = queries.reshape(TEXT, QUERY_HEAD_COUNT, HEAD_SIZE)
    mean_sq = lax.optimization_barrier(jnp.mean(shaped * shaped, axis=-1, keepdims=True))
    normed = (shaped * lax.rsqrt(mean_sq + 1e-05) * q_gain).astype(jnp.bfloat16)
    query_group_count = QUERY_HEAD_COUNT // KEY_VALUE_HEADS
    score_scale = 1.0 / HEAD_SIZE ** 0.5
    normed_wide = normed.astype(jnp.float32)

    def shard_step(state_carry, shard):
        key_block_offset = (shard * VISUAL_PER_CTX).astype(jnp.int32)
        key_tile_rows = lax.dynamic_slice_in_dim(visual_key_cache, key_block_offset, VISUAL_PER_CTX, 0).reshape(VISUAL_PER_CTX, KEY_VALUE_HEADS, HEAD_SIZE)
        value_tile_rows = lax.dynamic_slice_in_dim(visual_value_cache, key_block_offset, VISUAL_PER_CTX, 0).reshape(VISUAL_PER_CTX, KEY_VALUE_HEADS, HEAD_SIZE)
        key_wide = jnp.repeat(key_tile_rows, query_group_count, axis=1).astype(jnp.float32)
        value_wide = jnp.repeat(value_tile_rows, query_group_count, axis=1).astype(jnp.float32)
        segments = lax.dynamic_slice_in_dim(block_mask, (shard * (VISUAL_PER_CTX // SEG)).astype(jnp.int32), VISUAL_PER_CTX // SEG, 1)
        positions = key_block_offset + jnp.arange(VISUAL_PER_CTX, dtype=jnp.int32)
        allowed = (jnp.repeat(segments, SEG, axis=1) == 1) & (positions[None, :] < lengths[:, None])
        scores = jnp.einsum('rhd,khd->hrk', normed_wide, key_wide) * score_scale
        scores = jnp.where(allowed[None], scores, jnp.float32(-1e+30))
        block_max = lax.optimization_barrier(jnp.max(scores, axis=-1))
        weights = jnp.where(allowed[None], jnp.exp(scores - block_max[..., None]), jnp.float32(0.0))
        block_total = lax.optimization_barrier(jnp.sum(weights, axis=-1))
        block_num = jnp.einsum('hrk,khd->hrd', weights.astype(jnp.bfloat16).astype(jnp.float32), value_wide)
        old_num, old_max, old_total = state_carry
        highest = jnp.maximum(old_max, block_max)
        old_factor = jnp.exp(old_max - highest)
        new_factor = jnp.exp(block_max - highest)
        merged = (old_num * old_factor[..., None] + block_num * new_factor[..., None], highest, old_total * old_factor + block_total * new_factor)
        return (merged, None)
    start_state = (jnp.zeros((QUERY_HEAD_COUNT, TEXT, HEAD_SIZE), jnp.float32), jnp.full((QUERY_HEAD_COUNT, TEXT), -1e+30, jnp.float32), jnp.zeros((QUERY_HEAD_COUNT, TEXT), jnp.float32))
    final_state, unused = lax.scan(shard_step, start_state, jnp.arange(N_CTX, dtype=jnp.int32))
    numerator, row_max, total = final_state
    attended = (numerator / total[..., None]).astype(jnp.bfloat16)
    attended = jnp.transpose(attended, (1, 0, 2)).reshape(TEXT, QUERY_HEAD_COUNT * HEAD_SIZE)
    projected = jnp.dot(attended, o_weight, preferred_element_type=jnp.float32)
    return (text_states.astype(jnp.float32) + projected).astype(jnp.bfloat16)
```

```python
import functools

import jax
import jax.numpy as jnp
from jax import lax
from jax.experimental import pallas as pl
from jax.experimental.pallas import tpu as pltpu
from jax.sharding import PartitionSpec as P

F32, BF16, I16, I32 = jnp.float32, jnp.bfloat16, jnp.int16, jnp.int32
LANES = 128
CODE_TOP = 32000.0
LOW = -1e30
NO_SUM = -32000.0
VM = pl.BlockSpec(memory_space=pltpu.VMEM)
SM = pl.BlockSpec(memory_space=pltpu.SMEM)


def call(kernel, out_shape, args, flops=0, scratch=(), name=None):
    moved = sum(a.size * a.dtype.itemsize for a in args)
    moved += sum(o.size * o.dtype.itemsize for o in jax.tree.leaves(out_shape))
    return pl.pallas_call(
        kernel,
        out_shape=out_shape,
        in_specs=[SM] + [VM] * (len(args) - 1),
        out_specs=jax.tree.map(lambda _: VM, out_shape),
        scratch_shapes=list(scratch),
        cost_estimate=pl.CostEstimate(flops=int(flops), bytes_accessed=int(moved), transcendentals=0),
        name=name,
    )(*args)


def encode(x, lane, base):
    rows, width = x.shape
    extra = jnp.zeros((rows, LANES), I32)
    codes = []
    for h in range(width // LANES):
        part = x[:, h * LANES : (h + 1) * LANES]
        top = jnp.max(jnp.abs(part), axis=1, keepdims=True)
        power = jnp.clip(jnp.floor(jnp.log2(jnp.maximum(top, 1e-30))) + 1.0, -100.0, 100.0)
        scaled = part * (jnp.exp2(-power) * CODE_TOP)
        scaled = jnp.clip(jnp.round(scaled), -32767.0, 32767.0)
        codes.append(scaled.astype(I32).astype(I16))
        extra = jnp.where(lane == base + h, power.astype(I32), extra)
    return codes, extra


def decode(codes, extra, h, column=None):
    column = h if column is None else column
    power = extra[:, column : column + 1].astype(F32)
    return codes.astype(I32).astype(F32) * (jnp.exp2(power) * (1.0 / CODE_TOP))


def project_kernel(ids, x_ref, w_ref, out_ref):
    out_ref[...] = jnp.dot(x_ref[...], w_ref[...], preferred_element_type=F32)


def split_x_kernel(ids, keep_ref, got_ref, code_ref, own_ref):
    half = own_ref.shape[0]
    width = own_ref.shape[1]
    mine = pl.multiple_of(ids[1] * half, half)
    peer = pl.multiple_of((1 - ids[1]) * half, half)
    own_ref[...] = keep_ref[pl.ds(mine, half), :] + got_ref[pl.ds(mine, half), :]
    lane = lax.broadcasted_iota(I32, (half, LANES), 1)
    extra = jnp.zeros((half, LANES), I32)
    for h in range(width // LANES):
        cols = slice(h * LANES, (h + 1) * LANES)
        part = keep_ref[pl.ds(peer, half), cols] + got_ref[pl.ds(peer, half), cols]
        codes, more = encode(part, lane, h)
        code_ref[:, cols] = codes[0]
        extra = extra + more
    code_ref[:, width:] = extra.astype(I16)


def split_z_kernel(groups, ids, own_ref, got_ref, *outs):
    own_out, code_outs = outs[0], outs[1:]
    rows, width = own_out.shape
    heads = width // LANES
    total = own_ref.shape[1]
    lane = lax.broadcasted_iota(I32, (rows, LANES), 1)
    extra_in = got_ref[:, total:].astype(I32)
    for d in range(groups):
        group = ids[2] ^ d
        extra = jnp.zeros((rows, LANES), I32)
        for h in range(heads):
            at = pl.multiple_of(group * width + h * LANES, LANES)
            head = group * heads + h
            power = jnp.sum(jnp.where(lane == head, extra_in, 0), axis=1, keepdims=True).astype(F32)
            got = got_ref[:, pl.ds(at, LANES)].astype(I32).astype(F32) * (jnp.exp2(power) * (1.0 / CODE_TOP))
            part = own_ref[:, pl.ds(at, LANES)] + got
            cols = slice(h * LANES, (h + 1) * LANES)
            if d == 0:
                own_out[:, cols] = part
            else:
                codes, more = encode(part, lane, h)
                code_outs[d - 1][:, cols] = codes[0]
                extra = extra + more
        if d:
            code_outs[d - 1][:, width:] = extra.astype(I16)


def norm_kernel(ids, own_ref, gain_ref, *rest):
    got, out_ref = rest[:-1], rest[-1]
    rows, width = out_ref.shape
    gain = gain_ref[...]
    extras = [g[:, width:].astype(I32) for g in got]
    for h in range(width // LANES):
        cols = slice(h * LANES, (h + 1) * LANES)
        total = own_ref[:, cols]
        for g, extra in zip(got, extras):
            total = total + decode(g[:, cols], extra, h)
        mean_sq = jnp.mean(total * total, axis=1, keepdims=True)
        out_ref[:, cols] = (total * lax.rsqrt(mean_sq + 1e-05) * gain).astype(BF16)


def attend_kernel(blocks, heads, rel, ids, q_ref, k_ref, v_ref, bias_ref, *rest):
    kvs, outs = rest[: blocks - 1], rest[blocks - 1 :]
    rows = q_ref.shape[0]
    keys = k_ref.shape[0]
    scale = 1.4426950408889634 / LANES**0.5
    kv_col = pl.multiple_of(ids[2] * LANES, LANES)
    core, x = ids[0] ^ (rel & 1), ids[1] ^ (rel >> 1)
    row_at = pl.multiple_of((core * 2 + x) * rows, rows)
    stacked = jnp.concatenate([q_ref[:, h * LANES : (h + 1) * LANES] for h in range(heads)], axis=0)
    highs, sums, nums = [], [], []
    for b in range(blocks):
        if b == 0:
            key, value = k_ref[:, pl.ds(kv_col, LANES)], v_ref[:, pl.ds(kv_col, LANES)]
        else:
            key, value = kvs[b - 1][:keys, :], kvs[b - 1][keys : 2 * keys, :]
        raw = lax.dot_general(stacked, key, (((1,), (1,)), ((), ())), preferred_element_type=F32)
        bias = bias_ref[b, pl.ds(row_at, rows), :]
        scores = raw.reshape(heads, rows, keys) * scale + bias[None]
        high = jnp.maximum(jnp.max(scores, axis=-1, keepdims=True), -1e29)
        weights = jnp.exp2(scores - high)
        highs.append(high)
        sums.append(jnp.sum(weights, axis=-1, keepdims=True))
        weights = weights.astype(BF16).reshape(heads * rows, keys)
        nums.append(jnp.dot(weights, value, preferred_element_type=F32).reshape(heads, rows, LANES))
    top = functools.reduce(jnp.maximum, highs)
    factors = [jnp.exp2(h - top) for h in highs]
    total = functools.reduce(jnp.add, [s * f for s, f in zip(sums, factors)])
    num = functools.reduce(jnp.add, [n * f for n, f in zip(nums, factors)])
    some = total > 0.0
    out = num * jnp.where(some, 1.0 / jnp.where(some, total, 1.0), 0.0)
    level = jnp.where(some, top + jnp.log2(jnp.where(some, total, 1.0)), NO_SUM)
    if rel == 0:
        out_ref, level_ref = outs
        for h in range(heads):
            out_ref[:, h * LANES : (h + 1) * LANES] = out[h]
        lane = lax.broadcasted_iota(I32, (rows, LANES), 1)
        levels = jnp.zeros((rows, LANES), F32)
        for h in range(heads):
            levels = jnp.where(lane == h, level[h], levels)
        level_ref[...] = levels
        return
    (code_ref,) = outs
    lane = lax.broadcasted_iota(I32, (rows, LANES), 1)
    extra = jnp.zeros((rows, LANES), I32)
    for h in range(heads):
        codes, more = encode(out[h], lane, h)
        code_ref[:, h * LANES : (h + 1) * LANES] = codes[0]
        whole = jnp.round(level[h])
        fine = jnp.clip(jnp.round((level[h] - whole) * 65536.0), -32767.0, 32767.0)
        extra = extra + more
        extra = jnp.where(lane == heads + h, whole.astype(I32), extra)
        extra = jnp.where(lane == 2 * heads + h, fine.astype(I32), extra)
    code_ref[:, heads * LANES :] = extra.astype(I16)


def merge_kernel(heads, ids, own_ref, level_ref, *rest):
    got, out_ref = rest[:-1], rest[-1]
    width = heads * LANES
    extras = [g[:, width:].astype(I32) for g in got]
    for h in range(heads):
        cols = slice(h * LANES, (h + 1) * LANES)
        levels = [level_ref[:, h : h + 1]]
        parts = [own_ref[:, cols]]
        for g, extra in zip(got, extras):
            whole = extra[:, heads + h : heads + h + 1].astype(F32)
            fine = extra[:, 2 * heads + h : 2 * heads + h + 1].astype(F32)
            levels.append(whole + fine * (1.0 / 65536.0))
            parts.append(decode(g[:, cols], extra, h))
        top = functools.reduce(jnp.maximum, levels)
        shares = [jnp.exp2(level - top) for level in levels]
        total = functools.reduce(jnp.add, shares)
        num = functools.reduce(jnp.add, [p * s for p, s in zip(parts, shares)])
        out_ref[:, cols] = (num / total).astype(BF16)


def output_kernel(groups, ids, a_ref, b_ref, w_ref, keep_ref, code_ref):
    rows, width = a_ref.shape[2:]
    lane = lax.broadcasted_iota(I32, (rows, LANES), 1)
    send_own = ids[0] != ids[3]
    for xs in range(2):
        at = pl.multiple_of((ids[1] ^ xs) * rows, rows)
        sums = []
        for src in (a_ref, b_ref):
            total = None
            for d in range(groups):
                base = pl.multiple_of((ids[2] ^ d) * width, width)
                part = jnp.dot(src[xs, d], w_ref[pl.ds(base, width), :], preferred_element_type=F32)
                total = part if total is None else total + part
            sums.append(total)
        flag = jnp.full((rows, 1), send_own.astype(I32), I32) == 1
        send = jnp.where(flag, sums[0], sums[1])
        keep_ref[pl.ds(at, rows), :] = jnp.where(flag, sums[1], sums[0])
        codes, extra = encode(send, lane, 0)
        for h, code in enumerate(codes):
            code_ref[pl.ds(at, rows), h * LANES : (h + 1) * LANES] = code
        code_ref[pl.ds(at, rows), len(codes) * LANES :] = extra.astype(I16)


def finish_kernel(ids, keep_ref, got_ref, text_ref, out_ref):
    rows, width = out_ref.shape
    at = pl.multiple_of(ids[3] * rows, rows)
    extra = got_ref[:, width:].astype(I32)
    for h in range(width // LANES):
        cols = slice(h * LANES, (h + 1) * LANES)
        total = keep_ref[:, cols] + decode(got_ref[:, cols], extra, h)
        out_ref[:, cols] = (text_ref[pl.ds(at, rows), cols].astype(F32) + total).astype(BF16)


def fast_shards(text_states, q_weight, q_gain, key_cache, value_cache, block_mask, lengths, o_weight):
    ctx = lax.axis_size("ctx")
    text_rows, depth = text_states.shape
    columns = q_weight.shape[1]
    keys = key_cache.shape[0]
    groups = key_cache.shape[1] // LANES
    width = columns // groups
    heads = width // LANES
    rows = text_rows // 4
    half = text_rows // 2
    segments = block_mask.shape[1]
    me = lax.axis_index("ctx")
    core, x, z = me % 2, (me // 2) % 2, me // 4
    tp = lax.axis_index(("head", "tp"))
    ids = jnp.stack([core, x, z, tp]).astype(I32)

    def swap(value, bits):
        return lax.ppermute(value, "ctx", [(i, i ^ bits) for i in range(ctx)])

    mask_rows = jnp.pad(
        block_mask.T.astype(BF16).reshape(segments * text_rows // LANES, LANES),
        ((0, -(segments * text_rows // LANES) % 16), (0, 0)),
    )
    kvs = []
    for d in range(1, groups):
        at = (z ^ d) * LANES
        pack = jnp.concatenate(
            [
                lax.dynamic_slice_in_dim(key_cache, at, LANES, 1),
                lax.dynamic_slice_in_dim(value_cache, at, LANES, 1),
                mask_rows,
            ],
            axis=0,
        )
        kvs.append(swap(pack, 4 * d))

    struct = jax.ShapeDtypeStruct
    flops = 2 * half * depth * columns
    x_send = lax.dynamic_slice_in_dim(text_states, (1 - core) * half, half, 0)
    x_keep = lax.dynamic_slice_in_dim(text_states, core * half, half, 0)
    part_shape = struct((half, columns), F32)
    sent = call(project_kernel, part_shape, (ids, x_send, q_weight), flops, name="project_send")
    got = swap(sent, 1)
    kept = call(project_kernel, part_shape, (ids, x_keep, q_weight), flops, name="project_keep")
    code, own = call(
        split_x_kernel,
        (struct((rows, columns + LANES), I16), struct((rows, columns), F32)),
        (ids, kept, got),
        name="split_x",
    )
    got = swap(code, 2)
    own, *codes = call(
        functools.partial(split_z_kernel, groups),
        (struct((rows, width), F32),) + (struct((rows, width + LANES), I16),) * (groups - 1),
        (ids, own, got),
        name="split_z",
    )
    got = [swap(c, 4 * (d + 1)) for d, c in enumerate(codes)]
    normed = call(
        norm_kernel,
        struct((rows, width), BF16),
        (ids, own, q_gain.reshape(1, LANES), *got),
        name="norm",
    )

    queries = [normed] + [swap(normed, t) for t in range(1, 4)]
    seg_len = keys // segments
    biases = []
    for d in range(groups):
        if d == 0:
            mask = block_mask.T.astype(BF16)
        else:
            mask = kvs[d - 1][2 * keys : 2 * keys + segments * text_rows // LANES].reshape(segments, text_rows)
        positions = (((z ^ d) * 4 + x * 2 + core) * keys + jnp.arange(keys, dtype=I32))[None, :]
        seen = jnp.repeat(mask.T == 1, seg_len, axis=1) & (positions < lengths[:, None])
        biases.append(jnp.where(seen, F32(0.0), F32(LOW)))
    bias = jnp.stack(biases)
    outs = []
    attn_flops = 4 * rows * heads * keys * groups * LANES
    for rel in (1, 2, 3, 0):
        if rel:
            shape = struct((rows, width + LANES), I16)
        else:
            shape = (struct((rows, width), F32), struct((rows, LANES), F32))
        res = call(
            functools.partial(attend_kernel, groups, heads, rel),
            shape,
            (ids, queries[rel], key_cache, value_cache, bias, *kvs),
            attn_flops,
            name=f"attend_{rel}",
        )
        outs.append(swap(res, rel) if rel else res)
    attended = call(
        functools.partial(merge_kernel, heads),
        struct((rows, width), BF16),
        (ids, *outs[3], *outs[:3]),
        name="merge",
    )

    column = jnp.stack([attended] + [swap(attended, 4 * d) for d in range(1, groups)])
    plane = jnp.stack([column, swap(column, 2)])
    other = swap(plane, 1)
    out_cols = o_weight.shape[1]
    kept, code = call(
        functools.partial(output_kernel, groups),
        (struct((half, out_cols), F32), struct((half, out_cols + LANES), I16)),
        (ids, plane, other, o_weight),
        2 * text_rows * columns * out_cols,
        name="output",
    )
    got = lax.ppermute(code, ("head", "tp"), [(0, 1), (1, 0)])
    return call(
        finish_kernel, struct((half, out_cols), BF16), (ids, kept, got, text_states), name="finish"
    )


def plain_shards(
    text_states,
    q_weight,
    q_gain,
    visual_key_cache,
    visual_value_cache,
    block_mask,
    lengths,
    o_weight,
):
    text_rows = text_states.shape[0]
    columns = q_weight.shape[1]
    head_dim = q_gain.shape[0]
    query_heads = columns // head_dim
    kv_heads = visual_key_cache.shape[1] // head_dim
    query_group_count = query_heads // kv_heads
    row_block = text_states
    query_share = lax.psum_scatter(
        jnp.dot(row_block, q_weight, preferred_element_type=jnp.float32),
        "ctx",
        scatter_dimension=0,
        tiled=True,
    )
    shaped = query_share.reshape(query_share.shape[0], query_heads, head_dim)
    mean_sq = jnp.mean(shaped * shaped, axis=-1, keepdims=True)
    normed = shaped * lax.rsqrt(mean_sq + 1e-05) * q_gain
    queries = lax.all_gather(
        normed.reshape(query_share.shape[0], columns).astype(jnp.bfloat16),
        "ctx",
        axis=0,
        tiled=True,
    )
    keys_local = visual_key_cache.shape[0]
    segment_len = keys_local // block_mask.shape[1]
    key_block_offset = lax.axis_index("ctx") * keys_local
    positions = key_block_offset + jnp.arange(keys_local, dtype=jnp.int32)
    allowed = (jnp.repeat(block_mask, segment_len, axis=1) == 1) & (
        positions[None, :] < lengths[:, None]
    )
    score_scale = 1.0 / head_dim**0.5
    partial_nums = []
    partial_maxes = []
    partial_totals = []
    for q_head in range(query_heads):
        kv_head = q_head // query_group_count
        query_part = queries[:, q_head * head_dim : (q_head + 1) * head_dim]
        key_part = visual_key_cache[:, kv_head * head_dim : (kv_head + 1) * head_dim]
        value_part = visual_value_cache[:, kv_head * head_dim : (kv_head + 1) * head_dim]
        scores = (
            lax.dot_general(
                query_part, key_part, (((1,), (1,)), ((), ())), preferred_element_type=jnp.float32
            )
            * score_scale
        )
        scores = jnp.where(allowed, scores, jnp.float32(-1e30))
        local_max = jnp.max(scores, axis=1)
        weights = jnp.where(allowed, jnp.exp(scores - local_max[:, None]), jnp.float32(0.0))
        partial_totals.append(jnp.sum(weights, axis=1))
        partial_maxes.append(local_max)
        partial_nums.append(
            jnp.dot(weights.astype(jnp.bfloat16), value_part, preferred_element_type=jnp.float32)
        )
    local_num = jnp.concatenate(partial_nums, axis=1)
    local_max = jnp.stack(partial_maxes, axis=1)
    local_total = jnp.stack(partial_totals, axis=1)
    highest = lax.pmax(local_max, "ctx")
    factor = jnp.exp(local_max - highest)
    scaled_num = local_num * jnp.repeat(factor, head_dim, axis=1)
    scaled_total = local_total * factor
    owned_num, owned_total = (
        lax.psum_scatter(scaled_num, "ctx", scatter_dimension=0, tiled=True),
        lax.psum_scatter(scaled_total, "ctx", scatter_dimension=0, tiled=True),
    )
    owned = (owned_num / jnp.repeat(owned_total, head_dim, axis=1)).astype(jnp.bfloat16)
    attended = lax.all_gather(owned, "ctx", axis=0, tiled=True)
    rows_out = text_rows // lax.axis_size(("head", "tp"))
    row_block = attended
    summed = lax.psum_scatter(
        jnp.dot(row_block, o_weight, preferred_element_type=jnp.float32),
        ("head", "tp"),
        scatter_dimension=0,
        tiled=True,
    )
    residual = lax.dynamic_slice_in_dim(
        text_states, lax.axis_index(("head", "tp")) * rows_out, rows_out, 0
    )
    return (residual.astype(jnp.float32) + summed).astype(jnp.bfloat16)


def solution(mesh):
    in_specs = (
        P(None, "ctx"),
        P("ctx", ("head", "tp")),
        P(),
        P("ctx", ("head", "tp")),
        P("ctx", ("head", "tp")),
        P(None, "ctx"),
        P(),
        P(("head", "tp"), "ctx"),
    )
    out_specs = P(("head", "tp"), "ctx")
    ctx, halves = mesh.shape["ctx"], mesh.shape["head"] * mesh.shape["tp"]

    def shards(*args):
        text_rows = args[0].shape[0]
        groups = args[3].shape[1] // args[2].shape[0]
        fits = (
            args[2].shape[0] == LANES
            and halves == 2
            and groups & (groups - 1) == 0
            and ctx == 4 * groups
            and text_rows % 64 == 0
            and (args[5].shape[1] * text_rows) % LANES == 0
        )
        return (fast_shards if fits else plain_shards)(*args)

    return jax.shard_map(shards, mesh=mesh, in_specs=in_specs, out_specs=out_specs, check_vma=False)
```

```python
import functools

import jax
import jax.numpy as jnp
from jax import lax
from jax.experimental import pallas as pl
from jax.experimental.pallas import tpu as pltpu
from jax.sharding import PartitionSpec as P

F32, BF16, I16, I32 = jnp.float32, jnp.bfloat16, jnp.int16, jnp.int32
LANES = 128
CODE_TOP = 32000.0
LOW = -1e30
NO_SUM = -32000.0
VM = pl.BlockSpec(memory_space=pltpu.VMEM)
SM = pl.BlockSpec(memory_space=pltpu.SMEM)


def call(kernel, out_shape, args, flops=0, scratch=(), name=None):
    moved = sum(a.size * a.dtype.itemsize for a in args)
    moved += sum(o.size * o.dtype.itemsize for o in jax.tree.leaves(out_shape))
    return pl.pallas_call(
        kernel,
        out_shape=out_shape,
        in_specs=[SM] + [VM] * (len(args) - 1),
        out_specs=jax.tree.map(lambda _: VM, out_shape),
        scratch_shapes=list(scratch),
        cost_estimate=pl.CostEstimate(flops=int(flops), bytes_accessed=int(moved), transcendentals=0),
        name=name,
        compiler_params=pltpu.CompilerParams(vmem_limit_bytes=16 * 2**20),
    )(*args)


def encode(x, lane, base):
    rows, width = x.shape
    extra = jnp.zeros((rows, LANES), I32)
    codes = []
    for h in range(width // LANES):
        part = x[:, h * LANES : (h + 1) * LANES]
        top = jnp.max(jnp.abs(part), axis=1, keepdims=True)
        power = jnp.clip(jnp.floor(jnp.log2(jnp.maximum(top, 1e-30))) + 1.0, -100.0, 100.0)
        scaled = part * (jnp.exp2(-power) * CODE_TOP)
        scaled = jnp.clip(jnp.round(scaled), -32767.0, 32767.0)
        codes.append(scaled.astype(I32).astype(I16))
        extra = jnp.where(lane == base + h, power.astype(I32), extra)
    return codes, extra


def decode(codes, extra, h, column=None):
    column = h if column is None else column
    power = extra[:, column : column + 1].astype(F32)
    return codes.astype(I32).astype(F32) * (jnp.exp2(power) * (1.0 / CODE_TOP))


def project_kernel(ids, x_ref, w_ref, out_ref):
    out_ref[...] = jnp.dot(x_ref[...], w_ref[...], preferred_element_type=F32)


def split_x_kernel(ids, keep_ref, got_ref, code_ref, own_ref):
    half = own_ref.shape[0]
    width = own_ref.shape[1]
    mine = pl.multiple_of(ids[1] * half, half)
    peer = pl.multiple_of((1 - ids[1]) * half, half)
    own_ref[...] = keep_ref[pl.ds(mine, half), :] + got_ref[pl.ds(mine, half), :]
    lane = lax.broadcasted_iota(I32, (half, LANES), 1)
    extra = jnp.zeros((half, LANES), I32)
    for h in range(width // LANES):
        cols = slice(h * LANES, (h + 1) * LANES)
        part = keep_ref[pl.ds(peer, half), cols] + got_ref[pl.ds(peer, half), cols]
        codes, more = encode(part, lane, h)
        code_ref[:, cols] = codes[0]
        extra = extra + more
    code_ref[:, width:] = extra.astype(I16)


def split_z_kernel(groups, ids, own_ref, got_ref, *outs):
    own_out, code_outs = outs[0], outs[1:]
    rows, width = own_out.shape
    heads = width // LANES
    total = own_ref.shape[1]
    lane = lax.broadcasted_iota(I32, (rows, LANES), 1)
    extra_in = got_ref[:, total:].astype(I32)
    for d in range(groups):
        group = ids[2] ^ d
        extra = jnp.zeros((rows, LANES), I32)
        for h in range(heads):
            at = pl.multiple_of(group * width + h * LANES, LANES)
            head = group * heads + h
            power = jnp.sum(jnp.where(lane == head, extra_in, 0), axis=1, keepdims=True).astype(F32)
            got = got_ref[:, pl.ds(at, LANES)].astype(I32).astype(F32) * (jnp.exp2(power) * (1.0 / CODE_TOP))
            part = own_ref[:, pl.ds(at, LANES)] + got
            cols = slice(h * LANES, (h + 1) * LANES)
            if d == 0:
                own_out[:, cols] = part
            else:
                codes, more = encode(part, lane, h)
                code_outs[d - 1][:, cols] = codes[0]
                extra = extra + more
        if d:
            code_outs[d - 1][:, width:] = extra.astype(I16)


def norm_kernel(ids, own_ref, gain_ref, *rest):
    got, out_ref = rest[:-1], rest[-1]
    rows, width = out_ref.shape
    gain = gain_ref[...]
    extras = [g[:, width:].astype(I32) for g in got]
    for h in range(width // LANES):
        cols = slice(h * LANES, (h + 1) * LANES)
        total = own_ref[:, cols]
        for g, extra in zip(got, extras):
            total = total + decode(g[:, cols], extra, h)
        mean_sq = jnp.mean(total * total, axis=1, keepdims=True)
        out_ref[:, cols] = (total * lax.rsqrt(mean_sq + 1e-05) * gain).astype(BF16)


def attend_kernel(blocks, heads, rel, ids, q_ref, k_ref, v_ref, bias_ref, *rest):
    kvs, outs = rest[: blocks - 1], rest[blocks - 1 :]
    rows = q_ref.shape[0]
    keys = k_ref.shape[0]
    scale = 1.4426950408889634 / LANES**0.5
    kv_col = pl.multiple_of(ids[2] * LANES, LANES)
    core, x = ids[0] ^ (rel & 1), ids[1] ^ (rel >> 1)
    row_at = pl.multiple_of((core * 2 + x) * rows, rows)
    stacked = jnp.concatenate([q_ref[:, h * LANES : (h + 1) * LANES] for h in range(heads)], axis=0)
    highs, sums, nums = [], [], []
    for b in range(blocks):
        if b == 0:
            key, value = k_ref[:, pl.ds(kv_col, LANES)], v_ref[:, pl.ds(kv_col, LANES)]
        else:
            key, value = kvs[b - 1][:keys, :], kvs[b - 1][keys : 2 * keys, :]
        raw = lax.dot_general(stacked, key, (((1,), (1,)), ((), ())), preferred_element_type=F32)
        bias = bias_ref[b, pl.ds(row_at, rows), :]
        scores = raw.reshape(heads, rows, keys) * scale + bias[None]
        high = jnp.maximum(jnp.max(scores, axis=-1, keepdims=True), -1e29)
        weights = jnp.exp2(scores - high)
        highs.append(high)
        sums.append(jnp.sum(weights, axis=-1, keepdims=True))
        weights = weights.astype(BF16).reshape(heads * rows, keys)
        nums.append(jnp.dot(weights, value, preferred_element_type=F32).reshape(heads, rows, LANES))
    top = functools.reduce(jnp.maximum, highs)
    factors = [jnp.exp2(h - top) for h in highs]
    total = functools.reduce(jnp.add, [s * f for s, f in zip(sums, factors)])
    num = functools.reduce(jnp.add, [n * f for n, f in zip(nums, factors)])
    some = total > 0.0
    out = num * jnp.where(some, 1.0 / jnp.where(some, total, 1.0), 0.0)
    level = jnp.where(some, top + jnp.log2(jnp.where(some, total, 1.0)), NO_SUM)
    if rel == 0:
        out_ref, level_ref = outs
        for h in range(heads):
            out_ref[:, h * LANES : (h + 1) * LANES] = out[h]
        lane = lax.broadcasted_iota(I32, (rows, LANES), 1)
        levels = jnp.zeros((rows, LANES), F32)
        for h in range(heads):
            levels = jnp.where(lane == h, level[h], levels)
        level_ref[...] = levels
        return
    (code_ref,) = outs
    lane = lax.broadcasted_iota(I32, (rows, LANES), 1)
    extra = jnp.zeros((rows, LANES), I32)
    for h in range(heads):
        codes, more = encode(out[h], lane, h)
        code_ref[:, h * LANES : (h + 1) * LANES] = codes[0]
        whole = jnp.round(level[h])
        fine = jnp.clip(jnp.round((level[h] - whole) * 65536.0), -32767.0, 32767.0)
        extra = extra + more
        extra = jnp.where(lane == heads + h, whole.astype(I32), extra)
        extra = jnp.where(lane == 2 * heads + h, fine.astype(I32), extra)
    code_ref[:, heads * LANES :] = extra.astype(I16)


def merge_kernel(heads, ids, own_ref, level_ref, *rest):
    got, out_ref = rest[:-1], rest[-1]
    width = heads * LANES
    extras = [g[:, width:].astype(I32) for g in got]
    for h in range(heads):
        cols = slice(h * LANES, (h + 1) * LANES)
        levels = [level_ref[:, h : h + 1]]
        parts = [own_ref[:, cols]]
        for g, extra in zip(got, extras):
            whole = extra[:, heads + h : heads + h + 1].astype(F32)
            fine = extra[:, 2 * heads + h : 2 * heads + h + 1].astype(F32)
            levels.append(whole + fine * (1.0 / 65536.0))
            parts.append(decode(g[:, cols], extra, h))
        top = functools.reduce(jnp.maximum, levels)
        shares = [jnp.exp2(level - top) for level in levels]
        total = functools.reduce(jnp.add, shares)
        num = functools.reduce(jnp.add, [p * s for p, s in zip(parts, shares)])
        out_ref[:, cols] = (num / total).astype(BF16)


def output_kernel(groups, ids, a_ref, b_ref, w_ref, keep_ref, code_ref):
    rows, width = a_ref.shape[2:]
    lane = lax.broadcasted_iota(I32, (rows, LANES), 1)
    send_own = ids[0] != ids[3]
    for xs in range(2):
        at = pl.multiple_of((ids[1] ^ xs) * rows, rows)
        sums = []
        for src in (a_ref, b_ref):
            total = None
            for d in range(groups):
                base = pl.multiple_of((ids[2] ^ d) * width, width)
                part = jnp.dot(src[xs, d], w_ref[pl.ds(base, width), :], preferred_element_type=F32)
                total = part if total is None else total + part
            sums.append(total)
        flag = jnp.full((rows, 1), send_own.astype(I32), I32) == 1
        send = jnp.where(flag, sums[0], sums[1])
        keep_ref[pl.ds(at, rows), :] = jnp.where(flag, sums[1], sums[0])
        codes, extra = encode(send, lane, 0)
        for h, code in enumerate(codes):
            code_ref[pl.ds(at, rows), h * LANES : (h + 1) * LANES] = code
        code_ref[pl.ds(at, rows), len(codes) * LANES :] = extra.astype(I16)


def finish_kernel(ids, keep_ref, got_ref, text_ref, out_ref):
    rows, width = out_ref.shape
    at = pl.multiple_of(ids[3] * rows, rows)
    extra = got_ref[:, width:].astype(I32)
    for h in range(width // LANES):
        cols = slice(h * LANES, (h + 1) * LANES)
        total = keep_ref[:, cols] + decode(got_ref[:, cols], extra, h)
        out_ref[:, cols] = (text_ref[pl.ds(at, rows), cols].astype(F32) + total).astype(BF16)


def fast_shards(text_states, q_weight, q_gain, key_cache, value_cache, block_mask, lengths, o_weight):
    ctx = lax.axis_size("ctx")
    text_rows, depth = text_states.shape
    columns = q_weight.shape[1]
    keys = key_cache.shape[0]
    groups = key_cache.shape[1] // LANES
    width = columns // groups
    heads = width // LANES
    rows = text_rows // 4
    half = text_rows // 2
    segments = block_mask.shape[1]
    me = lax.axis_index("ctx")
    core, x, z = me % 2, (me // 2) % 2, me // 4
    tp = lax.axis_index(("head", "tp"))
    ids = jnp.stack([core, x, z, tp]).astype(I32)

    def swap(value, bits):
        return lax.ppermute(value, "ctx", [(i, i ^ bits) for i in range(ctx)])

    mask_rows = jnp.pad(
        block_mask.T.astype(BF16).reshape(segments * text_rows // LANES, LANES),
        ((0, -(segments * text_rows // LANES) % 16), (0, 0)),
    )
    kvs = []
    for d in range(1, groups):
        at = (z ^ d) * LANES
        pack = jnp.concatenate(
            [
                lax.dynamic_slice_in_dim(key_cache, at, LANES, 1),
                lax.dynamic_slice_in_dim(value_cache, at, LANES, 1),
                mask_rows,
            ],
            axis=0,
        )
        kvs.append(swap(pack, 4 * d))

    struct = jax.ShapeDtypeStruct
    flops = 2 * half * depth * columns
    x_send = lax.dynamic_slice_in_dim(text_states, (1 - core) * half, half, 0)
    x_keep = lax.dynamic_slice_in_dim(text_states, core * half, half, 0)
    part_shape = struct((half, columns), F32)
    sent = call(project_kernel, part_shape, (ids, x_send, q_weight), flops, name="project_send")
    got = swap(sent, 1)
    kept = call(project_kernel, part_shape, (ids, x_keep, q_weight), flops, name="project_keep")
    code, own = call(
        split_x_kernel,
        (struct((rows, columns + LANES), I16), struct((rows, columns), F32)),
        (ids, kept, got),
        name="split_x",
    )
    got = swap(code, 2)
    own, *codes = call(
        functools.partial(split_z_kernel, groups),
        (struct((rows, width), F32),) + (struct((rows, width + LANES), I16),) * (groups - 1),
        (ids, own, got),
        name="split_z",
    )
    got = [swap(c, 4 * (d + 1)) for d, c in enumerate(codes)]
    normed = call(
        norm_kernel,
        struct((rows, width), BF16),
        (ids, own, q_gain.reshape(1, LANES), *got),
        name="norm",
    )

    queries = [normed] + [swap(normed, t) for t in range(1, 4)]
    seg_len = keys // segments
    biases = []
    for d in range(groups):
        if d == 0:
            mask = block_mask.T.astype(BF16)
        else:
            mask = kvs[d - 1][2 * keys : 2 * keys + segments * text_rows // LANES].reshape(segments, text_rows)
        positions = (((z ^ d) * 4 + x * 2 + core) * keys + jnp.arange(keys, dtype=I32))[None, :]
        seen = jnp.repeat(mask.T == 1, seg_len, axis=1) & (positions < lengths[:, None])
        biases.append(jnp.where(seen, F32(0.0), F32(LOW)))
    bias = jnp.stack(biases)
    outs = []
    attn_flops = 4 * rows * heads * keys * groups * LANES
    for rel in (1, 2, 3, 0):
        if rel:
            shape = struct((rows, width + LANES), I16)
        else:
            shape = (struct((rows, width), F32), struct((rows, LANES), F32))
        res = call(
            functools.partial(attend_kernel, groups, heads, rel),
            shape,
            (ids, queries[rel], key_cache, value_cache, bias, *kvs),
            attn_flops,
            name=f"attend_{rel}",
        )
        outs.append(swap(res, rel) if rel else res)
    attended = call(
        functools.partial(merge_kernel, heads),
        struct((rows, width), BF16),
        (ids, *outs[3], *outs[:3]),
        name="merge",
    )

    column = jnp.stack([attended] + [swap(attended, 4 * d) for d in range(1, groups)])
    plane = jnp.stack([column, swap(column, 2)])
    other = swap(plane, 1)
    out_cols = o_weight.shape[1]
    kept, code = call(
        functools.partial(output_kernel, groups),
        (struct((half, out_cols), F32), struct((half, out_cols + LANES), I16)),
        (ids, plane, other, o_weight),
        2 * text_rows * columns * out_cols,
        name="output",
    )
    got = lax.ppermute(code, ("head", "tp"), [(0, 1), (1, 0)])
    return call(
        finish_kernel, struct((half, out_cols), BF16), (ids, kept, got, text_states), name="finish"
    )


def plain_shards(
    text_states,
    q_weight,
    q_gain,
    visual_key_cache,
    visual_value_cache,
    block_mask,
    lengths,
    o_weight,
):
    text_rows = text_states.shape[0]
    columns = q_weight.shape[1]
    head_dim = q_gain.shape[0]
    query_heads = columns // head_dim
    kv_heads = visual_key_cache.shape[1] // head_dim
    query_group_count = query_heads // kv_heads
    row_block = text_states
    query_share = lax.psum_scatter(
        jnp.dot(row_block, q_weight, preferred_element_type=jnp.float32),
        "ctx",
        scatter_dimension=0,
        tiled=True,
    )
    shaped = query_share.reshape(query_share.shape[0], query_heads, head_dim)
    mean_sq = jnp.mean(shaped * shaped, axis=-1, keepdims=True)
    normed = shaped * lax.rsqrt(mean_sq + 1e-05) * q_gain
    queries = lax.all_gather(
        normed.reshape(query_share.shape[0], columns).astype(jnp.bfloat16),
        "ctx",
        axis=0,
        tiled=True,
    )
    keys_local = visual_key_cache.shape[0]
    segment_len = keys_local // block_mask.shape[1]
    key_block_offset = lax.axis_index("ctx") * keys_local
    positions = key_block_offset + jnp.arange(keys_local, dtype=jnp.int32)
    allowed = (jnp.repeat(block_mask, segment_len, axis=1) == 1) & (
        positions[None, :] < lengths[:, None]
    )
    score_scale = 1.0 / head_dim**0.5
    partial_nums = []
    partial_maxes = []
    partial_totals = []
    for q_head in range(query_heads):
        kv_head = q_head // query_group_count
        query_part = queries[:, q_head * head_dim : (q_head + 1) * head_dim]
        key_part = visual_key_cache[:, kv_head * head_dim : (kv_head + 1) * head_dim]
        value_part = visual_value_cache[:, kv_head * head_dim : (kv_head + 1) * head_dim]
        scores = (
            lax.dot_general(
                query_part, key_part, (((1,), (1,)), ((), ())), preferred_element_type=jnp.float32
            )
            * score_scale
        )
        scores = jnp.where(allowed, scores, jnp.float32(-1e30))
        local_max = jnp.max(scores, axis=1)
        weights = jnp.where(allowed, jnp.exp(scores - local_max[:, None]), jnp.float32(0.0))
        partial_totals.append(jnp.sum(weights, axis=1))
        partial_maxes.append(local_max)
        partial_nums.append(
            jnp.dot(weights.astype(jnp.bfloat16), value_part, preferred_element_type=jnp.float32)
        )
    local_num = jnp.concatenate(partial_nums, axis=1)
    local_max = jnp.stack(partial_maxes, axis=1)
    local_total = jnp.stack(partial_totals, axis=1)
    highest = lax.pmax(local_max, "ctx")
    factor = jnp.exp(local_max - highest)
    scaled_num = local_num * jnp.repeat(factor, head_dim, axis=1)
    scaled_total = local_total * factor
    owned_num, owned_total = (
        lax.psum_scatter(scaled_num, "ctx", scatter_dimension=0, tiled=True),
        lax.psum_scatter(scaled_total, "ctx", scatter_dimension=0, tiled=True),
    )
    owned = (owned_num / jnp.repeat(owned_total, head_dim, axis=1)).astype(jnp.bfloat16)
    attended = lax.all_gather(owned, "ctx", axis=0, tiled=True)
    rows_out = text_rows // lax.axis_size(("head", "tp"))
    row_block = attended
    summed = lax.psum_scatter(
        jnp.dot(row_block, o_weight, preferred_element_type=jnp.float32),
        ("head", "tp"),
        scatter_dimension=0,
        tiled=True,
    )
    residual = lax.dynamic_slice_in_dim(
        text_states, lax.axis_index(("head", "tp")) * rows_out, rows_out, 0
    )
    return (residual.astype(jnp.float32) + summed).astype(jnp.bfloat16)


def solution(mesh):
    in_specs = (
        P(None, "ctx"),
        P("ctx", ("head", "tp")),
        P(),
        P("ctx", ("head", "tp")),
        P("ctx", ("head", "tp")),
        P(None, "ctx"),
        P(),
        P(("head", "tp"), "ctx"),
    )
    out_specs = P(("head", "tp"), "ctx")
    ctx, halves = mesh.shape["ctx"], mesh.shape["head"] * mesh.shape["tp"]

    def shards(*args):
        text_rows = args[0].shape[0]
        groups = args[3].shape[1] // args[2].shape[0]
        fits = (
            args[2].shape[0] == LANES
            and halves == 2
            and groups & (groups - 1) == 0
            and ctx == 4 * groups
            and text_rows % 64 == 0
            and (args[5].shape[1] * text_rows) % LANES == 0
        )
        return (fast_shards if fits else plain_shards)(*args)

    return jax.shard_map(shards, mesh=mesh, in_specs=in_specs, out_specs=out_specs, check_vma=False)
```

```python
import functools

import jax
import jax.numpy as jnp
from jax import lax
from jax.experimental import pallas as pl
from jax.experimental.pallas import tpu as pltpu
from jax.sharding import PartitionSpec as P

F32, BF16, I16, I32 = jnp.float32, jnp.bfloat16, jnp.int16, jnp.int32
LANES = 128
TAIL = 16
CODE_TOP = 32000.0
LOW = -1e30
NO_SUM = -32000.0
VM = pl.BlockSpec(memory_space=pltpu.VMEM)
SM = pl.BlockSpec(memory_space=pltpu.SMEM)
HB = pl.BlockSpec(memory_space=pltpu.HBM)


def call(kernel, out_shape, args, name, flops=0, specs=None, scratch=()):
    moved = sum(a.size * a.dtype.itemsize for a in args)
    moved += sum(o.size * o.dtype.itemsize for o in jax.tree.leaves(out_shape))
    return pl.pallas_call(
        kernel,
        out_shape=out_shape,
        in_specs=[SM] + (specs or [VM] * (len(args) - 1)),
        out_specs=jax.tree.map(lambda _: VM, out_shape),
        scratch_shapes=list(scratch),
        cost_estimate=pl.CostEstimate(flops=int(flops), bytes_accessed=int(moved), transcendentals=0),
        compiler_params=pltpu.CompilerParams(vmem_limit_bytes=16 * 2**20),
        name=name,
    )(*args)


def power_of(top):
    return jnp.floor(jnp.log2(jnp.maximum(top, 1e-30))) + 1.0


def encode_heads(parts, code_ref):
    rows = parts[0].shape[0]
    lane = lax.broadcasted_iota(I32, (rows, LANES), 1)
    tops = jnp.zeros((rows, LANES), F32)
    for h, part in enumerate(parts):
        tops = jnp.where(lane == h, jnp.max(jnp.abs(part), axis=1, keepdims=True), tops)
    power = power_of(tops)
    scale = jnp.exp2(-power) * CODE_TOP
    for h, part in enumerate(parts):
        code = jnp.round(part * scale[:, h : h + 1])
        code_ref[:, h * LANES : (h + 1) * LANES] = code.astype(I32).astype(I16)
    code_ref[:, len(parts) * LANES :] = power.astype(I32).astype(I16)


def scales_of(code_ref):
    width = code_ref.shape[1] - LANES
    return jnp.exp2(code_ref[:, width:].astype(I32).astype(F32)) * (1.0 / CODE_TOP)


def decode_head(code_ref, scales, h):
    return code_ref[:, h * LANES : (h + 1) * LANES].astype(I32).astype(F32) * scales[:, h : h + 1]


def pack_kernel(groups, ids, key_ref, value_ref, mask_ref, *outs):
    keys = key_ref.shape[0]
    for d in range(groups):
        at = pl.multiple_of((ids[2] ^ d) * LANES, LANES)
        outs[d][:keys, :] = key_ref[:, pl.ds(at, LANES)]
        outs[d][keys : 2 * keys, :] = jnp.concatenate(
            [
                jnp.transpose(value_ref[pl.ds(c * LANES, LANES), pl.ds(at, LANES)])
                for c in range(keys // LANES)
            ],
            axis=0,
        )
        outs[d][2 * keys :, :] = mask_ref[...]


def project_kernel(ds, ids, x_ref, w_hbm, send_ref, keep_ref, w_buf, sems):
    half = x_ref.shape[0] // 2
    width = w_buf.shape[2]
    copies = []
    for i, d in enumerate(ds):
        at = pl.multiple_of((ids[2] ^ d) * width, width)
        copies.append(pltpu.make_async_copy(w_hbm.at[:, pl.ds(at, width)], w_buf.at[i], sems.at[i]))
        copies[-1].start()
    peer = pl.multiple_of((1 - ids[0]) * half, half)
    mine = pl.multiple_of(ids[0] * half, half)
    for i in range(len(ds)):
        copies[i].wait()
        cols = slice(i * width, (i + 1) * width)
        w = w_buf[i]
        send_ref[:, cols] = jnp.dot(x_ref[pl.ds(peer, half), :], w, preferred_element_type=F32)
        keep_ref[:, cols] = jnp.dot(x_ref[pl.ds(mine, half), :], w, preferred_element_type=F32)


def split_x_kernel(ids, keep_ref, got_ref, code_ref, own_ref):
    half, width = own_ref.shape
    mine = pl.multiple_of(ids[1] * half, half)
    peer = pl.multiple_of((1 - ids[1]) * half, half)
    parts = []
    for h in range(width // LANES):
        cols = slice(h * LANES, (h + 1) * LANES)
        parts.append(keep_ref[pl.ds(peer, half), cols] + got_ref[pl.ds(peer, half), cols])
    encode_heads(parts, code_ref)
    own_ref[...] = keep_ref[pl.ds(mine, half), :] + got_ref[pl.ds(mine, half), :]


def split_z_kernel(ds, ids, own_ref, got_ref, *outs):
    heads = own_ref.shape[1] // len(ds) // LANES
    scales = scales_of(got_ref)
    for i, d in enumerate(ds):
        parts = []
        for h in range(i * heads, (i + 1) * heads):
            parts.append(own_ref[:, h * LANES : (h + 1) * LANES] + decode_head(got_ref, scales, h))
        if d:
            encode_heads(parts, outs[i])
        else:
            for h, part in enumerate(parts):
                outs[i][:, h * LANES : (h + 1) * LANES] = part


def norm_kernel(ids, own_ref, gain_ref, *rest):
    got, out_ref = rest[:-1], rest[-1]
    gain = gain_ref[...]
    scales = [scales_of(g) for g in got]
    for h in range(out_ref.shape[1] // LANES):
        cols = slice(h * LANES, (h + 1) * LANES)
        total = own_ref[:, cols]
        for g, scale in zip(got, scales):
            total = total + decode_head(g, scale, h)
        mean_sq = jnp.mean(total * total, axis=1, keepdims=True)
        out_ref[:, cols] = (total * lax.rsqrt(mean_sq + 1e-05) * gain).astype(BF16)


def attend_kernel(groups, heads, segments, rel, ids, q_ref, lens_ref, *rest):
    packs, outs = rest[:groups], rest[groups:]
    rows = q_ref.shape[0]
    keys = (packs[0].shape[0] - TAIL) // 2
    seg = keys // segments
    units = heads * rows // LANES
    scale = 1.4426950408889634 / LANES**0.5
    core, x = ids[0] ^ (rel & 1), ids[1] ^ (rel >> 1)
    low_lanes = lax.broadcasted_iota(I32, (8, LANES), 1) < rows
    take_low = jnp.full((8, LANES), 1 - x, I32) == 1

    def twice(row):
        wide = jnp.broadcast_to(row, (8, LANES))
        turned = pltpu.roll(wide, rows, 1)
        return jnp.where(take_low == low_lanes, wide, turned)[:1]

    lens = twice(jnp.where(core == 1, lens_ref[1:2, :], lens_ref[0:1, :]))
    stacked = jnp.concatenate([q_ref[:, h * LANES : (h + 1) * LANES] for h in range(heads)], axis=0)
    highs, sums, nums = [], [], []
    for b in range(groups):
        pack = packs[b]
        raw = lax.dot_general(pack[:keys, :], stacked, (((1,), (1,)), ((), ())), preferred_element_type=F32)
        tail = pack[2 * keys :, :].astype(F32)
        first = ((ids[2] ^ b) * 4 + ids[1] * 2 + ids[0]) * keys
        masks = []
        for s in range(segments):
            seen = twice(jnp.where(core == 1, tail[2 * s + 1 : 2 * s + 2, :], tail[2 * s : 2 * s + 1, :]))
            limit = jnp.where(seen > 0.5, lens - (first + s * seg), 0)
            inside = lax.broadcasted_iota(I32, (seg, LANES), 0) < limit
            masks.append(jnp.where(inside, F32(0.0), F32(LOW)))
        bias = jnp.concatenate(masks, axis=0)
        unit_highs, unit_sums, unit_weights = [], [], []
        for u in range(units):
            scores = raw[:, u * LANES : (u + 1) * LANES] * scale + bias
            high = jnp.maximum(jnp.max(scores, axis=0, keepdims=True), -1e29)
            weights = jnp.exp2(scores - high)
            unit_highs.append(high)
            unit_sums.append(jnp.sum(weights, axis=0, keepdims=True))
            unit_weights.append(weights.astype(BF16))
        highs.append(jnp.concatenate(unit_highs, axis=1))
        sums.append(jnp.concatenate(unit_sums, axis=1))
        value = jnp.concatenate(
            [pack[keys + c * LANES : keys + (c + 1) * LANES, :] for c in range(keys // LANES)], axis=1
        )
        nums.append(jnp.dot(value, jnp.concatenate(unit_weights, axis=1), preferred_element_type=F32))
    top = functools.reduce(jnp.maximum, highs)
    factors = [jnp.exp2(h - top) for h in highs]
    total = functools.reduce(jnp.add, [s * f for s, f in zip(sums, factors)])
    num = functools.reduce(jnp.add, [n * f for n, f in zip(nums, factors)])
    some = total > 0.0
    out = num * jnp.where(some, 1.0 / jnp.where(some, total, 1.0), 0.0)
    level = jnp.where(some, top + jnp.log2(jnp.where(some, total, 1.0)), NO_SUM)
    if rel == 0:
        out_ref, level_ref = outs
        out_ref[...] = out
        level_ref[...] = jnp.broadcast_to(level, level_ref.shape)
        return
    (code_ref,) = outs
    power = power_of(jnp.max(jnp.abs(out), axis=0, keepdims=True))
    code_ref[:LANES, :] = jnp.round(out * (jnp.exp2(-power) * CODE_TOP)).astype(I32).astype(I16)
    whole = jnp.round(level)
    fine = jnp.clip(jnp.round((level - whole) * 65536.0), -32767.0, 32767.0)
    line = lax.broadcasted_iota(I32, (TAIL, heads * rows), 0)
    tail = jnp.where(line == 0, power, jnp.where(line == 1, whole, jnp.where(line == 2, fine, 0.0)))
    code_ref[LANES:, :] = tail.astype(I32).astype(I16)


def merge_kernel(heads, ids, own_ref, level_ref, *rest):
    got, out_ref = rest[:-1], rest[-1]
    rows = out_ref.shape[0]
    tails = [g[LANES:, :].astype(I32).astype(F32) for g in got]
    levels = [level_ref[:1, :]] + [t[1:2] + t[2:3] * (1.0 / 65536.0) for t in tails]
    top = functools.reduce(jnp.maximum, levels)
    shares = [jnp.exp2(level - top) for level in levels]
    inverse = 1.0 / functools.reduce(jnp.add, shares)
    num = own_ref[...] * (shares[0] * inverse)
    for g, tail, share in zip(got, tails, shares[1:]):
        weight = jnp.exp2(tail[:1]) * (1.0 / CODE_TOP) * share * inverse
        num = num + g[:LANES, :].astype(I32).astype(F32) * weight
    per = LANES // rows
    for u in range(heads // per):
        block = jnp.transpose(num[:, u * LANES : (u + 1) * LANES])
        for p in range(per):
            h = u * per + p
            out_ref[:, h * LANES : (h + 1) * LANES] = block[p * rows : (p + 1) * rows].astype(BF16)


def output_part(ds, ids, blocks, w_ref):
    width = blocks[0][0].shape[1]
    total = None
    for d, row_blocks in zip(ds, blocks):
        left = jnp.concatenate([b[...] for b in row_blocks], axis=0)
        base = pl.multiple_of((ids[2] ^ d) * width, width)
        part = jnp.dot(left, w_ref[pl.ds(base, width), :], preferred_element_type=F32)
        total = part if total is None else total + part
    return total


def output_first_kernel(ds, ids, w_ref, *rest):
    blocks = [rest[4 * i : 4 * i + 4] for i in range(len(ds))]
    rest[-1][...] = output_part(ds, ids, blocks, w_ref)


def output_last_kernel(ds, ids, w_ref, before_ref, *rest):
    blocks, (keep_ref, code_ref, send_buf) = [rest[4 * i : 4 * i + 4] for i in range(len(ds))], rest[-3:]
    total = output_part(ds, ids, blocks, w_ref) + before_ref[...]
    rows = total.shape[0] // 4
    swap_core = jnp.full((rows, 1), (ids[0] == ids[3]).astype(I32), I32) == 1
    for xs in range(2):
        at = pl.multiple_of((ids[1] ^ xs) * rows, rows)
        own = total[xs * rows : (xs + 1) * rows]
        other = total[(2 + xs) * rows : (3 + xs) * rows]
        send_buf[pl.ds(at, rows), :] = jnp.where(swap_core, other, own)
        keep_ref[pl.ds(at, rows), :] = jnp.where(swap_core, own, other)
    width = send_buf.shape[1]
    encode_heads([send_buf[:, h * LANES : (h + 1) * LANES] for h in range(width // LANES)], code_ref)


def finish_kernel(ids, keep_ref, got_ref, text_ref, out_ref):
    rows, width = out_ref.shape
    at = pl.multiple_of(ids[3] * rows, rows)
    scales = scales_of(got_ref)
    for h in range(width // LANES):
        cols = slice(h * LANES, (h + 1) * LANES)
        total = keep_ref[:, cols] + decode_head(got_ref, scales, h)
        out_ref[:, cols] = (text_ref[pl.ds(at, rows), cols].astype(F32) + total).astype(BF16)


def fast_shards(text_states, q_weight, q_gain, key_cache, value_cache, block_mask, lengths, o_weight):
    ctx = lax.axis_size("ctx")
    struct = jax.ShapeDtypeStruct
    text_rows, depth = text_states.shape
    columns = q_weight.shape[1]
    keys = key_cache.shape[0]
    groups = key_cache.shape[1] // LANES
    width = columns // groups
    heads = width // LANES
    rows, half = text_rows // 4, text_rows // 2
    pairs = heads * rows
    segments = block_mask.shape[1]
    out_cols = o_weight.shape[1]
    me = lax.axis_index("ctx")
    tp = lax.axis_index(("head", "tp"))
    ids = jnp.stack([me % 2, (me // 2) % 2, me // 4, tp]).astype(I32)

    def swap(value, bits):
        return lax.ppermute(value, "ctx", [(i, i ^ bits) for i in range(ctx)])

    def z_swap(value, d):
        return swap(value, 4 * d)

    order = list(range(groups - 1, -1, -1))
    chunks = [order[: groups // 2], order[groups // 2 :]] if groups > 1 else [order]
    sums = {}
    staged = []
    for n, ds in enumerate(chunks):
        part = struct((half, len(ds) * width), F32)
        sent, kept = call(
            functools.partial(project_kernel, ds),
            (part, part),
            (ids, text_states, q_weight),
            f"project_{n}",
            flops=2 * text_rows * depth * len(ds) * width,
            specs=[VM, HB],
            scratch=[pltpu.VMEM((len(ds), depth, width), BF16), pltpu.SemaphoreType.DMA((len(ds),))],
        )
        staged.append((kept, swap(sent, 1)))

    lines = segments * text_rows // LANES
    mask_rows = jnp.pad(block_mask.T.astype(BF16).reshape(lines, LANES), ((0, TAIL - lines), (0, 0)))
    packs = call(
        functools.partial(pack_kernel, groups),
        (struct((2 * keys + TAIL, LANES), BF16),) * groups,
        (ids, key_cache, value_cache, mask_rows),
        "pack",
    )
    packs = [packs[0]] + [z_swap(packs[d], d) for d in range(1, groups)]

    for n, ds in enumerate(chunks):
        kept, got = staged[n]
        wide = len(ds) * width
        code, own = call(
            split_x_kernel,
            (struct((rows, wide + LANES), I16), struct((rows, wide), F32)),
            (ids, kept, got),
            f"split_x_{n}",
        )
        got = swap(code, 2)
        outs = call(
            functools.partial(split_z_kernel, ds),
            tuple(struct((rows, width + LANES), I16) if d else struct((rows, width), F32) for d in ds),
            (ids, own, got),
            f"split_z_{n}",
        )
        for d, out in zip(ds, outs):
            sums[d] = z_swap(out, d) if d else out
    normed = call(
        norm_kernel,
        struct((rows, width), BF16),
        (ids, sums[0], q_gain.reshape(1, LANES), *[sums[d] for d in range(1, groups)]),
        "norm",
    )

    lens = lengths.reshape(2, LANES)
    outs = {}
    queries = [normed] + [swap(normed, t) for t in range(1, 4)]
    for rel in (0, 2, 3, 1):
        if rel:
            shape = struct((LANES + TAIL, pairs), I16)
        else:
            shape = (struct((LANES, pairs), F32), struct((8, pairs), F32))
        res = call(
            functools.partial(attend_kernel, groups, heads, segments, rel),
            shape,
            (ids, queries[rel], lens, *packs),
            f"attend_{rel}",
            flops=4 * pairs * keys * groups * LANES,
        )
        outs[rel] = swap(res, rel) if rel else res
    attended = call(
        functools.partial(merge_kernel, heads),
        struct((rows, width), BF16),
        (ids, *outs[0], outs[1], outs[2], outs[3]),
        "merge",
    )

    column = {0: attended, **{d: z_swap(attended, d) for d in order if d}}
    beside = {d: swap(column[d], 2) for d in range(groups)}
    blocks = {}
    for d in range(groups):
        own = (column[d], beside[d])
        blocks[d] = own + tuple(swap(b, 1) for b in own)
    late = [d for d in range(groups) if d >= groups // 2]
    early = [d for d in range(groups) if d < groups // 2]
    first = call(
        functools.partial(output_first_kernel, early),
        struct((text_rows, out_cols), F32),
        (ids, o_weight, *[b for d in early for b in blocks[d]]),
        "output_first",
        flops=2 * text_rows * width * len(early) * out_cols,
    )
    kept, code = call(
        functools.partial(output_last_kernel, late),
        (struct((half, out_cols), F32), struct((half, out_cols + LANES), I16)),
        (ids, o_weight, first, *[b for d in late for b in blocks[d]]),
        "output_last",
        flops=2 * text_rows * width * len(late) * out_cols,
        scratch=[pltpu.VMEM((half, out_cols), F32)],
    )
    got = lax.ppermute(code, ("head", "tp"), [(0, 1), (1, 0)])
    return call(finish_kernel, struct((half, out_cols), BF16), (ids, kept, got, text_states), "finish")


def plain_shards(
    text_states,
    q_weight,
    q_gain,
    visual_key_cache,
    visual_value_cache,
    block_mask,
    lengths,
    o_weight,
):
    text_rows = text_states.shape[0]
    columns = q_weight.shape[1]
    head_dim = q_gain.shape[0]
    query_heads = columns // head_dim
    kv_heads = visual_key_cache.shape[1] // head_dim
    query_group_count = query_heads // kv_heads
    row_block = text_states
    query_share = lax.psum_scatter(
        jnp.dot(row_block, q_weight, preferred_element_type=jnp.float32),
        "ctx",
        scatter_dimension=0,
        tiled=True,
    )
    shaped = query_share.reshape(query_share.shape[0], query_heads, head_dim)
    mean_sq = jnp.mean(shaped * shaped, axis=-1, keepdims=True)
    normed = shaped * lax.rsqrt(mean_sq + 1e-05) * q_gain
    queries = lax.all_gather(
        normed.reshape(query_share.shape[0], columns).astype(jnp.bfloat16),
        "ctx",
        axis=0,
        tiled=True,
    )
    keys_local = visual_key_cache.shape[0]
    segment_len = keys_local // block_mask.shape[1]
    key_block_offset = lax.axis_index("ctx") * keys_local
    positions = key_block_offset + jnp.arange(keys_local, dtype=jnp.int32)
    allowed = (jnp.repeat(block_mask, segment_len, axis=1) == 1) & (
        positions[None, :] < lengths[:, None]
    )
    score_scale = 1.0 / head_dim**0.5
    partial_nums = []
    partial_maxes = []
    partial_totals = []
    for q_head in range(query_heads):
        kv_head = q_head // query_group_count
        query_part = queries[:, q_head * head_dim : (q_head + 1) * head_dim]
        key_part = visual_key_cache[:, kv_head * head_dim : (kv_head + 1) * head_dim]
        value_part = visual_value_cache[:, kv_head * head_dim : (kv_head + 1) * head_dim]
        scores = (
            lax.dot_general(
                query_part, key_part, (((1,), (1,)), ((), ())), preferred_element_type=jnp.float32
            )
            * score_scale
        )
        scores = jnp.where(allowed, scores, jnp.float32(-1e30))
        local_max = jnp.max(scores, axis=1)
        weights = jnp.where(allowed, jnp.exp(scores - local_max[:, None]), jnp.float32(0.0))
        partial_totals.append(jnp.sum(weights, axis=1))
        partial_maxes.append(local_max)
        partial_nums.append(
            jnp.dot(weights.astype(jnp.bfloat16), value_part, preferred_element_type=jnp.float32)
        )
    local_num = jnp.concatenate(partial_nums, axis=1)
    local_max = jnp.stack(partial_maxes, axis=1)
    local_total = jnp.stack(partial_totals, axis=1)
    highest = lax.pmax(local_max, "ctx")
    factor = jnp.exp(local_max - highest)
    scaled_num = local_num * jnp.repeat(factor, head_dim, axis=1)
    scaled_total = local_total * factor
    owned_num, owned_total = (
        lax.psum_scatter(scaled_num, "ctx", scatter_dimension=0, tiled=True),
        lax.psum_scatter(scaled_total, "ctx", scatter_dimension=0, tiled=True),
    )
    owned = (owned_num / jnp.repeat(owned_total, head_dim, axis=1)).astype(jnp.bfloat16)
    attended = lax.all_gather(owned, "ctx", axis=0, tiled=True)
    rows_out = text_rows // lax.axis_size(("head", "tp"))
    row_block = attended
    summed = lax.psum_scatter(
        jnp.dot(row_block, o_weight, preferred_element_type=jnp.float32),
        ("head", "tp"),
        scatter_dimension=0,
        tiled=True,
    )
    residual = lax.dynamic_slice_in_dim(
        text_states, lax.axis_index(("head", "tp")) * rows_out, rows_out, 0
    )
    return (residual.astype(jnp.float32) + summed).astype(jnp.bfloat16)


def solution(mesh):
    in_specs = (
        P(None, "ctx"),
        P("ctx", ("head", "tp")),
        P(),
        P("ctx", ("head", "tp")),
        P("ctx", ("head", "tp")),
        P(None, "ctx"),
        P(),
        P(("head", "tp"), "ctx"),
    )
    out_specs = P(("head", "tp"), "ctx")
    ctx, halves = mesh.shape["ctx"], mesh.shape["head"] * mesh.shape["tp"]

    def shards(*args):
        text_rows = args[0].shape[0]
        groups = args[3].shape[1] // args[2].shape[0]
        fits = (
            args[2].shape[0] == LANES
            and halves == 2
            and text_rows == 2 * LANES
            and groups > 1
            and groups & (groups - 1) == 0
            and ctx == 4 * groups
            and args[1].shape[1] % (groups * LANES) == 0
            and args[1].shape[1] // groups <= LANES * LANES
            and 2 * args[5].shape[1] <= TAIL
            and args[3].shape[0] % (args[5].shape[1] * LANES) == 0
        )
        return (fast_shards if fits else plain_shards)(*args)

    return jax.shard_map(shards, mesh=mesh, in_specs=in_specs, out_specs=out_specs, check_vma=False)
```

```python
import functools

import jax
import jax.numpy as jnp
from jax import lax
from jax.experimental import pallas as pl
from jax.experimental.pallas import tpu as pltpu
from jax.sharding import PartitionSpec as P


F32, BF16, I16, I32 = jnp.float32, jnp.bfloat16, jnp.int16, jnp.int32
LANES = 128
TAIL = 16
CODE_TOP = 32000.0
LOW = -1e30
NO_SUM = -32000.0
VM = pl.BlockSpec(memory_space=pltpu.VMEM)
HB = pl.BlockSpec(memory_space=pltpu.HBM)

PROJECT_GRANT = 16


class Position:
    def __getitem__(self, i):
        me = lax.axis_index("ctx")
        if i == 0:
            return lax.rem(me, 2)
        if i == 1:
            return lax.rem(lax.div(me, 2), 2)
        if i == 2:
            return lax.div(me, 4)
        return lax.axis_index("head") * lax.axis_size("tp") + lax.axis_index("tp")


ids = Position()


def call(kernel, out_shape, args, flops=0, specs=None, scratch=(), grant=16):
    moved = sum(a.size * a.dtype.itemsize for a in args)
    moved += sum(o.size * o.dtype.itemsize for o in jax.tree.leaves(out_shape))
    return pl.pallas_call(
        kernel,
        out_shape=out_shape,
        in_specs=specs or [VM] * len(args),
        out_specs=jax.tree.map(lambda _: VM, out_shape),
        scratch_shapes=list(scratch),
        cost_estimate=pl.CostEstimate(flops=int(flops), bytes_accessed=int(moved), transcendentals=0),
        compiler_params=pltpu.CompilerParams(vmem_limit_bytes=grant * 2**20),
    )(*args)


def power_of(top):
    return jnp.floor(jnp.log2(jnp.maximum(top, 1e-30))) + 1.0


def encode_heads(parts, code_ref):
    rows = parts[0].shape[0]
    lane = lax.broadcasted_iota(I32, (rows, LANES), 1)
    tops = jnp.zeros((rows, LANES), F32)
    for h, part in enumerate(parts):
        tops = jnp.where(lane == h, jnp.max(jnp.abs(part), axis=1, keepdims=True), tops)
    power = power_of(tops)
    scale = jnp.exp2(-power) * CODE_TOP
    for h, part in enumerate(parts):
        code = jnp.round(part * scale[:, h : h + 1])
        code_ref[:, h * LANES : (h + 1) * LANES] = code.astype(I32).astype(I16)
    code_ref[:, len(parts) * LANES :] = power.astype(I32).astype(I16)


def scales_of(code_ref):
    width = code_ref.shape[1] - LANES
    return jnp.exp2(code_ref[:, width:].astype(I32).astype(F32)) * (1.0 / CODE_TOP)


def decode_head(code_ref, scales, h):
    return code_ref[:, h * LANES : (h + 1) * LANES].astype(I32).astype(F32) * scales[:, h : h + 1]


def pack_kernel(groups, key_ref, value_ref, mask_ref, *outs):
    keys = key_ref.shape[0]
    for d in range(groups):
        at = pl.multiple_of((ids[2] ^ d) * LANES, LANES)
        outs[d][:keys, :] = key_ref[:, pl.ds(at, LANES)]
        outs[d][keys : 2 * keys, :] = jnp.concatenate(
            [
                jnp.transpose(value_ref[pl.ds(c * LANES, LANES), pl.ds(at, LANES)])
                for c in range(keys // LANES)
            ],
            axis=0,
        )
        outs[d][2 * keys :, :] = mask_ref[...]


def project_kernel(ds, x_ref, w_hbm, send_ref, keep_ref, w_buf, sems):
    half = x_ref.shape[0] // 2
    width = w_buf.shape[2]
    copies = []
    for i, d in enumerate(ds):
        at = pl.multiple_of((ids[2] ^ d) * width, width)
        copies.append(pltpu.make_async_copy(w_hbm.at[:, pl.ds(at, width)], w_buf.at[i], sems.at[i]))
        copies[-1].start()
    peer = pl.multiple_of((1 - ids[0]) * half, half)
    mine = pl.multiple_of(ids[0] * half, half)
    for i in range(len(ds)):
        copies[i].wait()
        cols = slice(i * width, (i + 1) * width)
        w = w_buf[i]
        send_ref[:, cols] = jnp.dot(x_ref[pl.ds(peer, half), :], w, preferred_element_type=F32)
        keep_ref[:, cols] = jnp.dot(x_ref[pl.ds(mine, half), :], w, preferred_element_type=F32)


def split_x_kernel(keep_ref, got_ref, code_ref, own_ref):
    half, width = own_ref.shape
    mine = pl.multiple_of(ids[1] * half, half)
    peer = pl.multiple_of((1 - ids[1]) * half, half)
    parts = []
    for h in range(width // LANES):
        cols = slice(h * LANES, (h + 1) * LANES)
        parts.append(keep_ref[pl.ds(peer, half), cols] + got_ref[pl.ds(peer, half), cols])
    encode_heads(parts, code_ref)
    own_ref[...] = keep_ref[pl.ds(mine, half), :] + got_ref[pl.ds(mine, half), :]


def split_z_kernel(ds, own_ref, got_ref, *outs):
    heads = own_ref.shape[1] // len(ds) // LANES
    scales = scales_of(got_ref)
    for i, d in enumerate(ds):
        parts = []
        for h in range(i * heads, (i + 1) * heads):
            parts.append(own_ref[:, h * LANES : (h + 1) * LANES] + decode_head(got_ref, scales, h))
        if d:
            encode_heads(parts, outs[i])
        else:
            for h, part in enumerate(parts):
                outs[i][:, h * LANES : (h + 1) * LANES] = part


def norm_kernel(own_ref, gain_ref, *rest):
    got, out_ref = rest[:-1], rest[-1]
    gain = gain_ref[...]
    scales = [scales_of(g) for g in got]
    for h in range(out_ref.shape[1] // LANES):
        cols = slice(h * LANES, (h + 1) * LANES)
        total = own_ref[:, cols]
        for g, scale in zip(got, scales):
            total = total + decode_head(g, scale, h)
        mean_sq = jnp.mean(total * total, axis=1, keepdims=True)
        out_ref[:, cols] = (total * lax.rsqrt(mean_sq + 1e-05) * gain).astype(BF16)


def attend_kernel(ds, heads, segments, rel, begin, finish, q_ref, lens_ref, *rest):
    packs, rest = rest[: len(ds)], rest[len(ds) :]
    state, outs = (None, rest) if begin else (rest[:2], rest[2:])
    rows = q_ref.shape[0]
    keys = (packs[0].shape[0] - TAIL) // 2
    seg = keys // segments
    units = heads * rows // LANES
    scale = 1.4426950408889634 / LANES**0.5
    core, x = ids[0] ^ (rel & 1), ids[1] ^ (rel >> 1)
    low_lanes = lax.broadcasted_iota(I32, (8, LANES), 1) < rows
    take_low = jnp.full((8, LANES), 1 - x, I32) == 1

    def twice(row):
        wide = jnp.broadcast_to(row, (8, LANES))
        turned = pltpu.roll(wide, rows, 1)
        return jnp.where(take_low == low_lanes, wide, turned)[:1]

    lens = twice(jnp.where(core == 1, lens_ref[1:2, :], lens_ref[0:1, :]))
    stacked = jnp.concatenate([q_ref[:, h * LANES : (h + 1) * LANES] for h in range(heads)], axis=0)
    highs, sums, nums = [], [], []
    for b, pack in zip(ds, packs):
        raw = lax.dot_general(pack[:keys, :], stacked, (((1,), (1,)), ((), ())), preferred_element_type=F32)
        tail = pack[2 * keys :, :].astype(F32)
        first = ((ids[2] ^ b) * 4 + ids[1] * 2 + ids[0]) * keys
        masks = []
        for s in range(segments):
            seen = twice(jnp.where(core == 1, tail[2 * s + 1 : 2 * s + 2, :], tail[2 * s : 2 * s + 1, :]))
            limit = jnp.where(seen > 0.5, lens - (first + s * seg), 0)
            inside = lax.broadcasted_iota(I32, (seg, LANES), 0) < limit
            masks.append(jnp.where(inside, F32(0.0), F32(LOW)))
        bias = jnp.concatenate(masks, axis=0)
        unit_highs, unit_sums, unit_weights = [], [], []
        for u in range(units):
            scores = raw[:, u * LANES : (u + 1) * LANES] * scale + bias
            high = jnp.maximum(jnp.max(scores, axis=0, keepdims=True), -1e29)
            weights = jnp.exp2(scores - high)
            unit_highs.append(high)
            unit_sums.append(jnp.sum(weights, axis=0, keepdims=True))
            unit_weights.append(weights.astype(BF16))
        highs.append(jnp.concatenate(unit_highs, axis=1))
        sums.append(jnp.concatenate(unit_sums, axis=1))
        value = jnp.concatenate(
            [pack[keys + c * LANES : keys + (c + 1) * LANES, :] for c in range(keys // LANES)], axis=1
        )
        nums.append(jnp.dot(value, jnp.concatenate(unit_weights, axis=1), preferred_element_type=F32))
    if not begin:
        highs.append(state[1][:1, :])
        sums.append(state[1][1:2, :])
        nums.append(state[0][...])
    top = functools.reduce(jnp.maximum, highs)
    factors = [jnp.exp2(h - top) for h in highs]
    total = functools.reduce(jnp.add, [s * f for s, f in zip(sums, factors)])
    num = functools.reduce(jnp.add, [n * f for n, f in zip(nums, factors)])
    if not finish:
        outs[0][...] = num
        line = lax.broadcasted_iota(I32, outs[1].shape, 0)
        outs[1][...] = jnp.where(line == 0, top, total)
        return
    some = total > 0.0
    out = num * jnp.where(some, 1.0 / jnp.where(some, total, 1.0), 0.0)
    level = jnp.where(some, top + jnp.log2(jnp.where(some, total, 1.0)), NO_SUM)
    if rel == 0:
        out_ref, level_ref = outs
        out_ref[...] = out
        level_ref[...] = jnp.broadcast_to(level, level_ref.shape)
        return
    (code_ref,) = outs
    power = power_of(jnp.max(jnp.abs(out), axis=0, keepdims=True))
    code_ref[:LANES, :] = jnp.round(out * (jnp.exp2(-power) * CODE_TOP)).astype(I32).astype(I16)
    whole = jnp.round(level)
    fine = jnp.clip(jnp.round((level - whole) * 65536.0), -32767.0, 32767.0)
    line = lax.broadcasted_iota(I32, (TAIL, heads * rows), 0)
    tail = jnp.where(line == 0, power, jnp.where(line == 1, whole, jnp.where(line == 2, fine, 0.0)))
    code_ref[LANES:, :] = tail.astype(I32).astype(I16)


def merge_kernel(heads, own_ref, level_ref, *rest):
    got, out_ref = rest[:-1], rest[-1]
    rows = out_ref.shape[0]
    tails = [g[LANES:, :].astype(I32).astype(F32) for g in got]
    levels = [level_ref[:1, :]] + [t[1:2] + t[2:3] * (1.0 / 65536.0) for t in tails]
    top = functools.reduce(jnp.maximum, levels)
    shares = [jnp.exp2(level - top) for level in levels]
    inverse = 1.0 / functools.reduce(jnp.add, shares)
    num = own_ref[...] * (shares[0] * inverse)
    for g, tail, share in zip(got, tails, shares[1:]):
        weight = jnp.exp2(tail[:1]) * (1.0 / CODE_TOP) * share * inverse
        num = num + g[:LANES, :].astype(I32).astype(F32) * weight
    per = LANES // rows
    for u in range(heads // per):
        block = jnp.transpose(num[:, u * LANES : (u + 1) * LANES])
        for p in range(per):
            h = u * per + p
            out_ref[:, h * LANES : (h + 1) * LANES] = block[p * rows : (p + 1) * rows].astype(BF16)


def output_part(ds, blocks, w_ref):
    width = blocks[0][0].shape[1]
    total = None
    for d, row_blocks in zip(ds, blocks):
        left = jnp.concatenate([b[...] for b in row_blocks], axis=0)
        base = pl.multiple_of((ids[2] ^ d) * width, width)
        part = jnp.dot(left, w_ref[pl.ds(base, width), :], preferred_element_type=F32)
        total = part if total is None else total + part
    return total


def output_first_kernel(ds, w_ref, *rest):
    blocks = [rest[4 * i : 4 * i + 4] for i in range(len(ds))]
    rest[-1][...] = output_part(ds, blocks, w_ref)


def output_last_kernel(ds, w_ref, before_ref, *rest):
    blocks, (keep_ref, code_ref, send_buf) = [rest[4 * i : 4 * i + 4] for i in range(len(ds))], rest[-3:]
    total = output_part(ds, blocks, w_ref) + before_ref[...]
    rows = total.shape[0] // 4
    swap_core = jnp.full((rows, 1), (ids[0] == ids[3]).astype(I32), I32) == 1
    for xs in range(2):
        at = pl.multiple_of((ids[1] ^ xs) * rows, rows)
        own = total[xs * rows : (xs + 1) * rows]
        other = total[(2 + xs) * rows : (3 + xs) * rows]
        send_buf[pl.ds(at, rows), :] = jnp.where(swap_core, other, own)
        keep_ref[pl.ds(at, rows), :] = jnp.where(swap_core, own, other)
    width = send_buf.shape[1]
    encode_heads([send_buf[:, h * LANES : (h + 1) * LANES] for h in range(width // LANES)], code_ref)


def finish_kernel(keep_ref, got_ref, text_ref, out_ref):
    rows, width = out_ref.shape
    at = pl.multiple_of(ids[3] * rows, rows)
    scales = scales_of(got_ref)
    for h in range(width // LANES):
        cols = slice(h * LANES, (h + 1) * LANES)
        total = keep_ref[:, cols] + decode_head(got_ref, scales, h)
        out_ref[:, cols] = (text_ref[pl.ds(at, rows), cols].astype(F32) + total).astype(BF16)


def fast_shards(text_states, q_weight, q_gain, key_cache, value_cache, block_mask, lengths, o_weight):
    ctx = lax.axis_size("ctx")
    struct = jax.ShapeDtypeStruct
    text_rows, depth = text_states.shape
    columns = q_weight.shape[1]
    keys = key_cache.shape[0]
    groups = key_cache.shape[1] // LANES
    width = columns // groups
    heads = width // LANES
    rows, half = text_rows // 4, text_rows // 2
    pairs = heads * rows
    segments = block_mask.shape[1]
    out_cols = o_weight.shape[1]

    def swap(value, bits):
        return lax.ppermute(value, "ctx", [(i, i ^ bits) for i in range(ctx)])

    def after(value, *others):
        return lax.optimization_barrier((value, *others))[0]

    lines = segments * text_rows // LANES
    mask_rows = jnp.pad(block_mask.T.astype(BF16).reshape(lines, LANES), ((0, TAIL - lines), (0, 0)))
    packs = call(
        functools.partial(pack_kernel, groups),
        (struct((2 * keys + TAIL, LANES), BF16),) * groups,
        (key_cache, value_cache, mask_rows),
    )
    packs = [packs[0]] + [swap(packs[d], 4 * d) for d in range(1, groups)]

    order = list(range(groups - 1, -1, -1))
    chunks = [[d] for d in order[: groups // 2]] + [order[groups // 2 :]]
    sums = {}
    text = text_states
    weight = pltpu.with_memory_space_constraint(q_weight, pltpu.HBM)
    for ds in chunks:
        wide = len(ds) * width
        part = struct((half, wide), F32)
        sent, kept = call(
            functools.partial(project_kernel, ds),
            (part, part),
            (text, weight),
            flops=2 * text_rows * depth * wide,
            specs=[VM, HB],
            scratch=[pltpu.VMEM((len(ds), depth, width), BF16), pltpu.SemaphoreType.DMA((len(ds),))],
            grant=PROJECT_GRANT,
        )
        got = swap(sent, 1)
        code, own = call(split_x_kernel, (struct((rows, wide + LANES), I16), struct((rows, wide), F32)), (kept, got))
        text = after(text_states, code)
        got = swap(code, 2)
        outs = call(
            functools.partial(split_z_kernel, ds),
            tuple(struct((rows, width + LANES), I16) if d else struct((rows, width), F32) for d in ds),
            (own, got),
        )
        for d, out in zip(ds, outs):
            sums[d] = swap(out, 4 * d) if d else out
    normed = call(
        norm_kernel,
        struct((rows, width), BF16),
        (sums[0], q_gain.reshape(1, LANES), *[sums[d] for d in range(1, groups)]),
    )

    lens = lengths.reshape(2, LANES)
    last = groups // 2
    first = [d for d in order[::-1] if d != last]
    queries = {t: swap(normed, t) if t else normed for t in range(4)}
    turns = (0, 2, 3, 1)
    states, previous = {}, ()
    for rel in turns:
        states[rel] = call(
            functools.partial(attend_kernel, first, heads, segments, rel, True, False),
            (struct((LANES, pairs), F32), struct((8, pairs), F32)),
            (after(queries[rel], *previous), lens, *[packs[d] for d in first]),
            flops=4 * pairs * keys * len(first) * LANES,
        )
        previous = states[rel]
    outs = {}
    for rel in turns[1:] + turns[:1]:
        if rel:
            shape = struct((LANES + TAIL, pairs), I16)
        else:
            shape = (struct((LANES, pairs), F32), struct((8, pairs), F32))
        res = call(
            functools.partial(attend_kernel, [last], heads, segments, rel, False, True),
            shape,
            (after(queries[rel], previous), lens, packs[last], *states[rel]),
            flops=4 * pairs * keys * LANES,
        )
        previous = res
        outs[rel] = swap(res, rel) if rel else res
    attended = call(
        functools.partial(merge_kernel, heads), struct((rows, width), BF16), (*outs[0], outs[1], outs[2], outs[3])
    )

    column = {d: swap(attended, 4 * d) if d else attended for d in order}
    beside = {d: swap(column[d], 2) for d in range(groups)}
    early, late = list(range(groups // 2)), list(range(groups // 2, groups))
    tail_d = late[0]

    def over_core(values):
        if len(values) == 1:
            return [swap(values[0], 1)]
        moved = swap(jnp.stack(values), 1)
        return [moved[i] for i in range(len(values))]

    blocks = {}
    moved = over_core([b for d in early for b in (column[d], beside[d])])
    for i, d in enumerate(early):
        blocks[d] = (column[d], beside[d], moved[2 * i], moved[2 * i + 1])
    pairs_late = [(d, side) for d in reversed(late) for side in (column, beside)][:-1]
    moved = over_core([side[d] for d, side in pairs_late])
    end = over_core([beside[tail_d]])
    moved = moved + end
    for i, d in enumerate(reversed(late)):
        blocks[d] = (column[d], beside[d], moved[2 * i], moved[2 * i + 1])
    before = call(
        functools.partial(output_first_kernel, early),
        struct((text_rows, out_cols), F32),
        (o_weight, *[b for d in early for b in blocks[d]]),
        flops=2 * text_rows * width * len(early) * out_cols,
    )
    kept, code = call(
        functools.partial(output_last_kernel, late),
        (struct((half, out_cols), F32), struct((half, out_cols + LANES), I16)),
        (o_weight, before, *[b for d in late for b in blocks[d]]),
        flops=2 * text_rows * width * len(late) * out_cols,
        scratch=[pltpu.VMEM((half, out_cols), F32)],
    )
    got = lax.ppermute(code, ("head", "tp"), [(0, 1), (1, 0)])
    return call(finish_kernel, struct((half, out_cols), BF16), (kept, got, text_states))


def plain_shards(
    text_states,
    q_weight,
    q_gain,
    visual_key_cache,
    visual_value_cache,
    block_mask,
    lengths,
    o_weight,
):
    text_rows = text_states.shape[0]
    columns = q_weight.shape[1]
    head_dim = q_gain.shape[0]
    query_heads = columns // head_dim
    kv_heads = visual_key_cache.shape[1] // head_dim
    query_group_count = query_heads // kv_heads
    row_block = text_states
    query_share = lax.psum_scatter(
        jnp.dot(row_block, q_weight, preferred_element_type=jnp.float32),
        "ctx",
        scatter_dimension=0,
        tiled=True,
    )
    shaped = query_share.reshape(query_share.shape[0], query_heads, head_dim)
    mean_sq = jnp.mean(shaped * shaped, axis=-1, keepdims=True)
    normed = shaped * lax.rsqrt(mean_sq + 1e-05) * q_gain
    queries = lax.all_gather(
        normed.reshape(query_share.shape[0], columns).astype(jnp.bfloat16),
        "ctx",
        axis=0,
        tiled=True,
    )
    keys_local = visual_key_cache.shape[0]
    segment_len = keys_local // block_mask.shape[1]
    key_block_offset = lax.axis_index("ctx") * keys_local
    positions = key_block_offset + jnp.arange(keys_local, dtype=jnp.int32)
    allowed = (jnp.repeat(block_mask, segment_len, axis=1) == 1) & (
        positions[None, :] < lengths[:, None]
    )
    score_scale = 1.0 / head_dim**0.5
    partial_nums = []
    partial_maxes = []
    partial_totals = []
    for q_head in range(query_heads):
        kv_head = q_head // query_group_count
        query_part = queries[:, q_head * head_dim : (q_head + 1) * head_dim]
        key_part = visual_key_cache[:, kv_head * head_dim : (kv_head + 1) * head_dim]
        value_part = visual_value_cache[:, kv_head * head_dim : (kv_head + 1) * head_dim]
        scores = (
            lax.dot_general(
                query_part, key_part, (((1,), (1,)), ((), ())), preferred_element_type=jnp.float32
            )
            * score_scale
        )
        scores = jnp.where(allowed, scores, jnp.float32(-1e30))
        local_max = jnp.max(scores, axis=1)
        weights = jnp.where(allowed, jnp.exp(scores - local_max[:, None]), jnp.float32(0.0))
        partial_totals.append(jnp.sum(weights, axis=1))
        partial_maxes.append(local_max)
        partial_nums.append(
            jnp.dot(weights.astype(jnp.bfloat16), value_part, preferred_element_type=jnp.float32)
        )
    local_num = jnp.concatenate(partial_nums, axis=1)
    local_max = jnp.stack(partial_maxes, axis=1)
    local_total = jnp.stack(partial_totals, axis=1)
    highest = lax.pmax(local_max, "ctx")
    factor = jnp.exp(local_max - highest)
    scaled_num = local_num * jnp.repeat(factor, head_dim, axis=1)
    scaled_total = local_total * factor
    owned_num, owned_total = (
        lax.psum_scatter(scaled_num, "ctx", scatter_dimension=0, tiled=True),
        lax.psum_scatter(scaled_total, "ctx", scatter_dimension=0, tiled=True),
    )
    owned = (owned_num / jnp.repeat(owned_total, head_dim, axis=1)).astype(jnp.bfloat16)
    attended = lax.all_gather(owned, "ctx", axis=0, tiled=True)
    rows_out = text_rows // lax.axis_size(("head", "tp"))
    row_block = attended
    summed = lax.psum_scatter(
        jnp.dot(row_block, o_weight, preferred_element_type=jnp.float32),
        ("head", "tp"),
        scatter_dimension=0,
        tiled=True,
    )
    residual = lax.dynamic_slice_in_dim(
        text_states, lax.axis_index(("head", "tp")) * rows_out, rows_out, 0
    )
    return (residual.astype(jnp.float32) + summed).astype(jnp.bfloat16)


def solution(mesh):
    in_specs = (
        P(None, "ctx"),
        P("ctx", ("head", "tp")),
        P(),
        P("ctx", ("head", "tp")),
        P("ctx", ("head", "tp")),
        P(None, "ctx"),
        P(),
        P(("head", "tp"), "ctx"),
    )
    out_specs = P(("head", "tp"), "ctx")
    ctx, halves = mesh.shape["ctx"], mesh.shape["head"] * mesh.shape["tp"]

    def fits(args):
        text_rows = args[0].shape[0]
        groups = args[3].shape[1] // args[2].shape[0]
        return (
            args[2].shape[0] == LANES
            and halves == 2
            and text_rows == 2 * LANES
            and groups > 1
            and groups & (groups - 1) == 0
            and ctx == 4 * groups
            and args[1].shape[1] % (groups * LANES) == 0
            and args[1].shape[1] // groups <= LANES * LANES
            and 2 * args[5].shape[1] <= TAIL
            and args[3].shape[0] % (args[5].shape[1] * LANES) == 0
        )

    def shards(*args):
        if not fits(args):
            return plain_shards(*args)
        return fast_shards(*args)

    spread = jax.shard_map(shards, mesh=mesh, in_specs=in_specs, out_specs=out_specs, check_vma=False)
    if halves != 2 or ctx != 16:
        return spread
    return spread
```

```python
import functools

import jax
import jax.numpy as jnp
from jax import lax
from jax.experimental import pallas as pl
from jax.experimental.pallas import tpu as pltpu
from jax.sharding import PartitionSpec as P


F32, BF16, I16, I32 = jnp.float32, jnp.bfloat16, jnp.int16, jnp.int32
LANES = 128
TAIL = 16
CODE_TOP = 32000.0
LOW = -1e30
NO_SUM = -32000.0
VM = pl.BlockSpec(memory_space=pltpu.VMEM)
HB = pl.BlockSpec(memory_space=pltpu.HBM)


class Position:
    def __getitem__(self, i):
        me = lax.axis_index("ctx")
        if i == 0:
            return lax.rem(me, 2)
        if i == 1:
            return lax.rem(lax.div(me, 2), 2)
        if i == 2:
            return lax.div(me, 4)
        return lax.axis_index("head") * lax.axis_size("tp") + lax.axis_index("tp")


ids = Position()


def call(kernel, out_shape, args, flops=0, specs=None, scratch=(), grant=16):
    moved = sum(a.size * a.dtype.itemsize for a in args)
    moved += sum(o.size * o.dtype.itemsize for o in jax.tree.leaves(out_shape))
    return pl.pallas_call(
        kernel,
        out_shape=out_shape,
        in_specs=specs or [VM] * len(args),
        out_specs=jax.tree.map(lambda _: VM, out_shape),
        scratch_shapes=list(scratch),
        cost_estimate=pl.CostEstimate(flops=int(flops), bytes_accessed=int(moved), transcendentals=0),
        compiler_params=pltpu.CompilerParams(vmem_limit_bytes=grant * 2**20),
    )(*args)


def power_of(top):
    return jnp.floor(jnp.log2(jnp.maximum(top, 1e-30))) + 1.0


def encode_heads(parts, code_ref):
    rows = parts[0].shape[0]
    lane = lax.broadcasted_iota(I32, (rows, LANES), 1)
    tops = jnp.zeros((rows, LANES), F32)
    for h, part in enumerate(parts):
        tops = jnp.where(lane == h, jnp.max(jnp.abs(part), axis=1, keepdims=True), tops)
    power = power_of(tops)
    scale = jnp.exp2(-power) * CODE_TOP
    for h, part in enumerate(parts):
        code = jnp.round(part * scale[:, h : h + 1])
        code_ref[h * rows : (h + 1) * rows, :] = code.astype(I32).astype(I16)
    square = jnp.concatenate([power, jnp.zeros((LANES - rows, LANES), F32)], axis=0)
    code_ref[len(parts) * rows :, :] = jnp.transpose(square)[:TAIL].astype(I32).astype(I16)


def scales_of(code_ref, rows):
    lines = code_ref[code_ref.shape[0] - TAIL :, :].astype(I32).astype(F32)
    square = jnp.concatenate([lines, jnp.zeros((LANES - TAIL, LANES), F32)], axis=0)
    return jnp.exp2(jnp.transpose(square)[:rows]) * (1.0 / CODE_TOP)


def decode_head(code_ref, scales, h):
    rows = scales.shape[0]
    return code_ref[h * rows : (h + 1) * rows, :].astype(I32).astype(F32) * scales[:, h : h + 1]


def begin_kernel(ds, x_hbm, w_hbm, key_hbm, value_hbm, mask_hbm, *rest):
    groups = len(ds)
    first, other, packs = rest[:2], rest[2:4], rest[4 : 4 + groups]
    x_ref, w_buf, key_ref, value_ref, mask_ref, sems = rest[4 + groups :]
    half = x_ref.shape[0] // 2
    width = w_buf.shape[2]
    keys = key_ref.shape[0]

    def fetch(source, target, n):
        copy = pltpu.make_async_copy(source, target, sems.at[n])
        copy.start()
        return copy

    def weights(i):
        at = pl.multiple_of((ids[2] ^ ds[i]) * width, width)
        return fetch(w_hbm.at[:, pl.ds(at, width)], w_buf.at[i], i)

    text = fetch(x_hbm, x_ref, groups)
    copies = [weights(0)]
    tokens = [fetch(key_hbm, key_ref, groups + 1), fetch(value_hbm, value_ref, groups + 2)]
    tokens.append(fetch(mask_hbm, mask_ref, groups + 3))
    copies += [weights(i) for i in range(1, groups)]
    peer = pl.multiple_of((1 - ids[0]) * half, half)
    mine = pl.multiple_of(ids[0] * half, half)

    def project(i, send_ref, keep_ref, at):
        copies[i].wait()
        cols = slice(at * width, (at + 1) * width)
        w = w_buf[i]
        send_ref[:, cols] = jnp.dot(x_ref[pl.ds(peer, half), :], w, preferred_element_type=F32)
        keep_ref[:, cols] = jnp.dot(x_ref[pl.ds(mine, half), :], w, preferred_element_type=F32)

    text.wait()
    project(0, *first, 0)
    for copy in tokens:
        copy.wait()
    line = lax.broadcasted_iota(I32, (TAIL, LANES), 0)
    tail = jnp.zeros((TAIL, LANES), F32)
    segments, text_rows = mask_ref.shape
    for s in range(segments):
        for j in range(text_rows // LANES):
            row = mask_ref[s : s + 1, j * LANES : (j + 1) * LANES]
            here = line == s * (text_rows // LANES) + j
            tail = jnp.where(here & (row == 1), F32(1.0), tail)
    for d in range(groups):
        at = pl.multiple_of((ids[2] ^ d) * LANES, LANES)
        packs[d][:keys, :] = key_ref[:, pl.ds(at, LANES)]
        for c in range(keys // LANES):
            block = value_ref[c * LANES : (c + 1) * LANES, pl.ds(at, LANES)]
            packs[d][keys + c * LANES : keys + (c + 1) * LANES, :] = jnp.transpose(block)
        packs[d][2 * keys :, :] = tail.astype(BF16)
    for i in range(1, groups):
        project(i, *other, i - 1)


def split_x_kernel(first, keep_ref, got_ref, code_ref, own_ref):
    half, width = own_ref.shape
    first *= width
    mine = pl.multiple_of(ids[1] * half, half)
    peer = pl.multiple_of((1 - ids[1]) * half, half)
    parts = []
    for h in range(width // LANES):
        cols = slice(first + h * LANES, first + (h + 1) * LANES)
        parts.append(keep_ref[pl.ds(peer, half), cols] + got_ref[pl.ds(peer, half), cols])
    encode_heads(parts, code_ref)
    cols = slice(first, first + width)
    own_ref[...] = keep_ref[pl.ds(mine, half), cols] + got_ref[pl.ds(mine, half), cols]


def split_z_kernel(ds, own_ref, got_ref, *outs):
    heads = own_ref.shape[1] // len(ds) // LANES
    scales = scales_of(got_ref, own_ref.shape[0])
    for i, d in enumerate(ds):
        parts = []
        for h in range(i * heads, (i + 1) * heads):
            parts.append(own_ref[:, h * LANES : (h + 1) * LANES] + decode_head(got_ref, scales, h))
        if d:
            encode_heads(parts, outs[i])
        else:
            for h, part in enumerate(parts):
                outs[i][:, h * LANES : (h + 1) * LANES] = part


def norm_kernel(own_ref, gain_ref, *rest):
    got, out_ref = rest[:-1], rest[-1]
    gain = gain_ref[...]
    scales = [scales_of(g, own_ref.shape[0]) for g in got]
    for h in range(out_ref.shape[1] // LANES):
        cols = slice(h * LANES, (h + 1) * LANES)
        total = own_ref[:, cols]
        for g, scale in zip(got, scales):
            total = total + decode_head(g, scale, h)
        mean_sq = jnp.mean(total * total, axis=1, keepdims=True)
        out_ref[:, cols] = (total * lax.rsqrt(mean_sq + 1e-05) * gain).astype(BF16)


def attend_kernel(ds, heads, segments, rel, begin, finish, q_ref, lens_ref, *rest):
    packs, rest = rest[: len(ds)], rest[len(ds) :]
    state, outs = (None, rest) if begin else (rest[:2], rest[2:])
    rows = q_ref.shape[0]
    keys = (packs[0].shape[0] - TAIL) // 2
    seg = keys // segments
    units = heads * rows // LANES
    scale = 1.4426950408889634 / LANES**0.5
    core, x = ids[0] ^ (rel & 1), ids[1] ^ (rel >> 1)
    low_lanes = lax.broadcasted_iota(I32, (8, LANES), 1) < rows
    take_low = jnp.full((8, LANES), 1 - x, I32) == 1

    def twice(row):
        wide = jnp.broadcast_to(row, (8, LANES))
        turned = pltpu.roll(wide, rows, 1)
        return jnp.where(take_low == low_lanes, wide, turned)[:1]

    lens = twice(jnp.where(core == 1, lens_ref[1:2, :], lens_ref[0:1, :]))
    stacked = jnp.concatenate([q_ref[:, h * LANES : (h + 1) * LANES] for h in range(heads)], axis=0)
    highs, sums, nums = [], [], []
    for b, pack in zip(ds, packs):
        raw = lax.dot_general(pack[:keys, :], stacked, (((1,), (1,)), ((), ())), preferred_element_type=F32)
        tail = pack[2 * keys :, :].astype(F32)
        first = ((ids[2] ^ b) * 4 + ids[1] * 2 + ids[0]) * keys
        masks = []
        for s in range(segments):
            seen = twice(jnp.where(core == 1, tail[2 * s + 1 : 2 * s + 2, :], tail[2 * s : 2 * s + 1, :]))
            limit = jnp.where(seen > 0.5, lens - (first + s * seg), 0)
            inside = lax.broadcasted_iota(I32, (seg, LANES), 0) < limit
            masks.append(jnp.where(inside, F32(0.0), F32(LOW)))
        bias = jnp.concatenate(masks, axis=0)
        unit_highs, unit_sums, unit_weights = [], [], []
        for u in range(units):
            scores = raw[:, u * LANES : (u + 1) * LANES] * scale + bias
            high = jnp.maximum(jnp.max(scores, axis=0, keepdims=True), -1e29)
            weights = jnp.exp2(scores - high)
            unit_highs.append(high)
            unit_sums.append(jnp.sum(weights, axis=0, keepdims=True))
            unit_weights.append(weights.astype(BF16))
        highs.append(jnp.concatenate(unit_highs, axis=1))
        sums.append(jnp.concatenate(unit_sums, axis=1))
        value = jnp.concatenate(
            [pack[keys + c * LANES : keys + (c + 1) * LANES, :] for c in range(keys // LANES)], axis=1
        )
        nums.append(jnp.dot(value, jnp.concatenate(unit_weights, axis=1), preferred_element_type=F32))
    if not begin:
        highs.append(state[1][:1, :])
        sums.append(state[1][1:2, :])
        nums.append(state[0][...])
    top = functools.reduce(jnp.maximum, highs)
    factors = [jnp.exp2(h - top) for h in highs]
    total = functools.reduce(jnp.add, [s * f for s, f in zip(sums, factors)])
    num = functools.reduce(jnp.add, [n * f for n, f in zip(nums, factors)])
    if not finish:
        outs[0][...] = num
        line = lax.broadcasted_iota(I32, outs[1].shape, 0)
        outs[1][...] = jnp.where(line == 0, top, total)
        return
    some = total > 0.0
    out = num * jnp.where(some, 1.0 / jnp.where(some, total, 1.0), 0.0)
    level = jnp.where(some, top + jnp.log2(jnp.where(some, total, 1.0)), NO_SUM)
    if rel == 0:
        out_ref, level_ref = outs
        out_ref[...] = out
        level_ref[...] = jnp.broadcast_to(level, level_ref.shape)
        return
    (code_ref,) = outs
    power = power_of(jnp.max(jnp.abs(out), axis=0, keepdims=True))
    code_ref[:LANES, :] = jnp.round(out * (jnp.exp2(-power) * CODE_TOP)).astype(I32).astype(I16)
    whole = jnp.round(level)
    fine = jnp.clip(jnp.round((level - whole) * 65536.0), -32767.0, 32767.0)
    line = lax.broadcasted_iota(I32, (TAIL, heads * rows), 0)
    tail = jnp.where(line == 0, power, jnp.where(line == 1, whole, jnp.where(line == 2, fine, 0.0)))
    code_ref[LANES:, :] = tail.astype(I32).astype(I16)


def merge_kernel(heads, own_ref, level_ref, *rest):
    got, out_ref = rest[:-1], rest[-1]
    rows = out_ref.shape[0]
    tails = [g[LANES:, :].astype(I32).astype(F32) for g in got]
    levels = [level_ref[:1, :]] + [t[1:2] + t[2:3] * (1.0 / 65536.0) for t in tails]
    top = functools.reduce(jnp.maximum, levels)
    shares = [jnp.exp2(level - top) for level in levels]
    inverse = 1.0 / functools.reduce(jnp.add, shares)
    num = own_ref[...] * (shares[0] * inverse)
    for g, tail, share in zip(got, tails, shares[1:]):
        weight = jnp.exp2(tail[:1]) * (1.0 / CODE_TOP) * share * inverse
        num = num + g[:LANES, :].astype(I32).astype(F32) * weight
    per = LANES // rows
    for u in range(heads // per):
        block = jnp.transpose(num[:, u * LANES : (u + 1) * LANES])
        for p in range(per):
            h = u * per + p
            out_ref[:, h * LANES : (h + 1) * LANES] = block[p * rows : (p + 1) * rows].astype(BF16)


def output_part(ds, blocks, w_ref):
    width = blocks[0][0].shape[1]
    total = None
    for d, row_blocks in zip(ds, blocks):
        left = jnp.concatenate([b[...] for b in row_blocks], axis=0)
        groups = w_ref.shape[0] // width
        base = pl.multiple_of(lax.rem(ids[2] + groups - d, groups) * width, width)
        part = jnp.dot(left, w_ref[pl.ds(base, width), :], preferred_element_type=F32)
        total = part if total is None else total + part
    return total


def output_first_kernel(ds, w_ref, *rest):
    blocks = [rest[4 * i : 4 * i + 4] for i in range(len(ds))]
    rest[-1][...] = output_part(ds, blocks, w_ref)


def output_last_kernel(ds, w_ref, before_ref, *rest):
    blocks, (keep_ref, code_ref, send_buf) = [rest[4 * i : 4 * i + 4] for i in range(len(ds))], rest[-3:]
    total = output_part(ds, blocks, w_ref) + before_ref[...]
    rows = total.shape[0] // 4
    swap_core = jnp.full((rows, 1), (ids[0] == ids[3]).astype(I32), I32) == 1
    for xs in range(2):
        at = pl.multiple_of((ids[1] ^ xs) * rows, rows)
        own = total[xs * rows : (xs + 1) * rows]
        other = total[(2 + xs) * rows : (3 + xs) * rows]
        send_buf[pl.ds(at, rows), :] = jnp.where(swap_core, other, own)
        keep_ref[pl.ds(at, rows), :] = jnp.where(swap_core, own, other)
    width = send_buf.shape[1]
    send = send_buf[...]
    power = power_of(jnp.max(jnp.abs(send), axis=0, keepdims=True))
    code_ref[: 2 * rows, :] = jnp.round(send * (jnp.exp2(-power) * CODE_TOP)).astype(I32).astype(I16)
    code_ref[2 * rows :, :] = jnp.broadcast_to(power, (TAIL, width)).astype(I32).astype(I16)


def finish_kernel(keep_ref, got_ref, text_ref, out_ref):
    rows = out_ref.shape[0]
    at = pl.multiple_of(ids[3] * rows, rows)
    scale = jnp.exp2(got_ref[rows:, :].astype(I32).astype(F32)[:1]) * (1.0 / CODE_TOP)
    total = keep_ref[...] + got_ref[:rows, :].astype(I32).astype(F32) * scale
    out_ref[...] = (text_ref[pl.ds(at, rows), :].astype(F32) + total).astype(BF16)


def fast_shards(text_states, q_weight, q_gain, key_cache, value_cache, block_mask, lengths, o_weight):
    ctx = lax.axis_size("ctx")
    struct = jax.ShapeDtypeStruct
    text_rows, depth = text_states.shape
    columns = q_weight.shape[1]
    keys = key_cache.shape[0]
    groups = key_cache.shape[1] // LANES
    width = columns // groups
    heads = width // LANES
    rows, half = text_rows // 4, text_rows // 2
    pairs = heads * rows
    segments = block_mask.shape[1]
    out_cols = o_weight.shape[1]

    def swap(value, bits):
        return lax.ppermute(value, "ctx", [(i, i ^ bits) for i in range(ctx)])

    def turn(value, shift):
        return lax.ppermute(value, "ctx", [(i, (i + shift) % ctx) for i in range(ctx)])

    def after(value, *others):
        return lax.optimization_barrier((value, *others))[0]

    in_hbm = functools.partial(pltpu.with_memory_space_constraint, memory_space=pltpu.HBM)
    order = list(range(groups - 1, -1, -1))
    chunks = [groups - 1, *[d for d in range(1, groups - 1)], 0]
    parts = [struct((half, width), F32)] * 2 + [struct((half, (groups - 1) * width), F32)] * 2
    sent, kept, sent_more, kept_more, *packs = call(
        functools.partial(begin_kernel, chunks),
        (*parts, *[struct((2 * keys + TAIL, LANES), BF16)] * groups),
        (in_hbm(text_states), in_hbm(q_weight), in_hbm(key_cache), in_hbm(value_cache), in_hbm(block_mask.T)),
        flops=2 * text_rows * depth * columns,
        specs=[HB] * 5,
        scratch=[
            pltpu.VMEM(text_states.shape, BF16),
            pltpu.VMEM((groups, depth, width), BF16),
            pltpu.VMEM(key_cache.shape, BF16),
            pltpu.VMEM(value_cache.shape, BF16),
            pltpu.VMEM((segments, text_rows), I32),
            pltpu.SemaphoreType.DMA((groups + 4,)),
        ],
    )
    packs = [packs[0]] + [swap(packs[d], 4 * d) for d in range(1, groups)]
    halves = (kept, swap(sent, 1))
    more = (kept_more, swap(sent_more, 1))

    sums = {}
    for n, d in enumerate(chunks):
        code, own = call(
            functools.partial(split_x_kernel, max(n - 1, 0)),
            (struct((pairs + TAIL, LANES), I16), struct((rows, width), F32)),
            more if n else halves,
        )
        got = swap(code, 2)
        (out,) = call(
            functools.partial(split_z_kernel, [d]),
            (struct((pairs + TAIL, LANES), I16) if d else struct((rows, width), F32),),
            (own, got),
        )
        sums[d] = swap(out, 4 * d) if d else out
    normed = call(
        norm_kernel,
        struct((rows, width), BF16),
        (sums[0], q_gain.reshape(1, LANES), *[sums[d] for d in range(1, groups)]),
    )

    lens = lengths.reshape(2, LANES)
    last = groups // 2
    first = [d for d in order[::-1] if d != last]
    queries = {t: swap(normed, t) if t else normed for t in range(4)}
    states, previous = {}, ()
    for rel in range(4):
        states[rel] = call(
            functools.partial(attend_kernel, first, heads, segments, rel, True, False),
            (struct((LANES, pairs), F32), struct((8, pairs), F32)),
            (after(queries[rel], *previous), lens, *[packs[d] for d in first]),
            flops=4 * pairs * keys * len(first) * LANES,
        )
        previous = states[rel]
    outs = {}
    for rel in (2, 3, 1, 0):
        if rel:
            shape = struct((LANES + TAIL, pairs), I16)
        else:
            shape = (struct((LANES, pairs), F32), struct((8, pairs), F32))
        res = call(
            functools.partial(attend_kernel, [last], heads, segments, rel, False, True),
            shape,
            (after(queries[rel], previous), lens, packs[last], *states[rel]),
            flops=4 * pairs * keys * LANES,
        )
        previous = res
        outs[rel] = swap(res, rel) if rel else res
    attended = call(
        functools.partial(merge_kernel, heads), struct((rows, width), BF16), (*outs[0], outs[1], outs[2], outs[3])
    )

    column = {d: turn(attended, 4 * d) if d else attended for d in order}
    beside = {d: swap(column[d], 2) for d in range(groups)}
    early, late = list(range(groups // 2)), list(range(groups // 2, groups))
    tail_d = late[0]

    def over_core(values):
        if len(values) == 1:
            return [swap(values[0], 1)]
        moved = swap(jnp.stack(values), 1)
        return [moved[i] for i in range(len(values))]

    blocks = {}
    moved = over_core([b for d in early for b in (column[d], beside[d])])
    for i, d in enumerate(early):
        blocks[d] = (column[d], beside[d], moved[2 * i], moved[2 * i + 1])
    pairs_late = [(d, side) for d in reversed(late) for side in (column, beside)][:-1]
    moved = over_core([side[d] for d, side in pairs_late])
    end = over_core([beside[tail_d]])
    moved = moved + end
    for i, d in enumerate(reversed(late)):
        blocks[d] = (column[d], beside[d], moved[2 * i], moved[2 * i + 1])
    before = call(
        functools.partial(output_first_kernel, early),
        struct((text_rows, out_cols), F32),
        (o_weight, *[b for d in early for b in blocks[d]]),
        flops=2 * text_rows * width * len(early) * out_cols,
    )
    kept, code = call(
        functools.partial(output_last_kernel, late),
        (struct((half, out_cols), F32), struct((half + TAIL, out_cols), I16)),
        (o_weight, before, *[b for d in late for b in blocks[d]]),
        flops=2 * text_rows * width * len(late) * out_cols,
        scratch=[pltpu.VMEM((half, out_cols), F32)],
    )
    got = lax.ppermute(code, ("head", "tp"), [(0, 1), (1, 0)])
    return call(finish_kernel, struct((half, out_cols), BF16), (kept, got, text_states))


def plain_shards(
    text_states,
    q_weight,
    q_gain,
    visual_key_cache,
    visual_value_cache,
    block_mask,
    lengths,
    o_weight,
):
    text_rows = text_states.shape[0]
    columns = q_weight.shape[1]
    head_dim = q_gain.shape[0]
    query_heads = columns // head_dim
    kv_heads = visual_key_cache.shape[1] // head_dim
    query_group_count = query_heads // kv_heads
    row_block = text_states
    query_share = lax.psum_scatter(
        jnp.dot(row_block, q_weight, preferred_element_type=jnp.float32),
        "ctx",
        scatter_dimension=0,
        tiled=True,
    )
    shaped = query_share.reshape(query_share.shape[0], query_heads, head_dim)
    mean_sq = jnp.mean(shaped * shaped, axis=-1, keepdims=True)
    normed = shaped * lax.rsqrt(mean_sq + 1e-05) * q_gain
    queries = lax.all_gather(
        normed.reshape(query_share.shape[0], columns).astype(jnp.bfloat16),
        "ctx",
        axis=0,
        tiled=True,
    )
    keys_local = visual_key_cache.shape[0]
    segment_len = keys_local // block_mask.shape[1]
    key_block_offset = lax.axis_index("ctx") * keys_local
    positions = key_block_offset + jnp.arange(keys_local, dtype=jnp.int32)
    allowed = (jnp.repeat(block_mask, segment_len, axis=1) == 1) & (
        positions[None, :] < lengths[:, None]
    )
    score_scale = 1.0 / head_dim**0.5
    partial_nums = []
    partial_maxes = []
    partial_totals = []
    for q_head in range(query_heads):
        kv_head = q_head // query_group_count
        query_part = queries[:, q_head * head_dim : (q_head + 1) * head_dim]
        key_part = visual_key_cache[:, kv_head * head_dim : (kv_head + 1) * head_dim]
        value_part = visual_value_cache[:, kv_head * head_dim : (kv_head + 1) * head_dim]
        scores = (
            lax.dot_general(
                query_part, key_part, (((1,), (1,)), ((), ())), preferred_element_type=jnp.float32
            )
            * score_scale
        )
        scores = jnp.where(allowed, scores, jnp.float32(-1e30))
        local_max = jnp.max(scores, axis=1)
        weights = jnp.where(allowed, jnp.exp(scores - local_max[:, None]), jnp.float32(0.0))
        partial_totals.append(jnp.sum(weights, axis=1))
        partial_maxes.append(local_max)
        partial_nums.append(
            jnp.dot(weights.astype(jnp.bfloat16), value_part, preferred_element_type=jnp.float32)
        )
    local_num = jnp.concatenate(partial_nums, axis=1)
    local_max = jnp.stack(partial_maxes, axis=1)
    local_total = jnp.stack(partial_totals, axis=1)
    highest = lax.pmax(local_max, "ctx")
    factor = jnp.exp(local_max - highest)
    scaled_num = local_num * jnp.repeat(factor, head_dim, axis=1)
    scaled_total = local_total * factor
    owned_num, owned_total = (
        lax.psum_scatter(scaled_num, "ctx", scatter_dimension=0, tiled=True),
        lax.psum_scatter(scaled_total, "ctx", scatter_dimension=0, tiled=True),
    )
    owned = (owned_num / jnp.repeat(owned_total, head_dim, axis=1)).astype(jnp.bfloat16)
    attended = lax.all_gather(owned, "ctx", axis=0, tiled=True)
    rows_out = text_rows // lax.axis_size(("head", "tp"))
    row_block = attended
    summed = lax.psum_scatter(
        jnp.dot(row_block, o_weight, preferred_element_type=jnp.float32),
        ("head", "tp"),
        scatter_dimension=0,
        tiled=True,
    )
    residual = lax.dynamic_slice_in_dim(
        text_states, lax.axis_index(("head", "tp")) * rows_out, rows_out, 0
    )
    return (residual.astype(jnp.float32) + summed).astype(jnp.bfloat16)


def solution(mesh):
    in_specs = (
        P(None, "ctx"),
        P("ctx", ("head", "tp")),
        P(),
        P("ctx", ("head", "tp")),
        P("ctx", ("head", "tp")),
        P(None, "ctx"),
        P(),
        P(("head", "tp"), "ctx"),
    )
    out_specs = P(("head", "tp"), "ctx")
    ctx, halves = mesh.shape["ctx"], mesh.shape["head"] * mesh.shape["tp"]

    def fits(args):
        text_rows = args[0].shape[0]
        groups = args[3].shape[1] // args[2].shape[0]
        return (
            args[2].shape[0] == LANES
            and halves == 2
            and text_rows == 2 * LANES
            and groups == 4
            and ctx == 4 * groups
            and args[1].shape[1] % (groups * LANES) == 0
            and args[1].shape[1] // groups <= LANES * LANES
            and 2 * args[5].shape[1] <= TAIL
            and args[3].shape[0] % (args[5].shape[1] * LANES) == 0
        )

    def shards(*args):
        if not fits(args):
            return plain_shards(*args)
        return fast_shards(*args)

    spread = jax.shard_map(shards, mesh=mesh, in_specs=in_specs, out_specs=out_specs, check_vma=False)
    if halves != 2 or ctx != 16:
        return spread
    return spread
```

```python
import functools

import jax
import jax.numpy as jnp
from jax import lax
from jax.experimental import pallas as pl
from jax.experimental.pallas import tpu as pltpu
from jax.sharding import PartitionSpec as P


F32, BF16, I16, I32 = jnp.float32, jnp.bfloat16, jnp.int16, jnp.int32
LANES = 128
TAIL = 16
CODE_TOP = 32000.0
LOW = -1e30
NO_SUM = -32000.0
VM = pl.BlockSpec(memory_space=pltpu.VMEM)
HB = pl.BlockSpec(memory_space=pltpu.HBM)


class Position:
    def __getitem__(self, i):
        me = lax.axis_index("ctx")
        if i == 0:
            return lax.rem(me, 2)
        if i == 1:
            return lax.rem(lax.div(me, 2), 2)
        if i == 2:
            return lax.div(me, 4)
        return lax.axis_index("head") * lax.axis_size("tp") + lax.axis_index("tp")


ids = Position()


def call(kernel, out_shape, args, flops=0, specs=None, scratch=(), grant=16):
    moved = sum(a.size * a.dtype.itemsize for a in args)
    moved += sum(o.size * o.dtype.itemsize for o in jax.tree.leaves(out_shape))
    return pl.pallas_call(
        kernel,
        out_shape=out_shape,
        in_specs=specs or [VM] * len(args),
        out_specs=jax.tree.map(lambda _: VM, out_shape),
        scratch_shapes=list(scratch),
        cost_estimate=pl.CostEstimate(flops=int(flops), bytes_accessed=int(moved), transcendentals=0),
        compiler_params=pltpu.CompilerParams(vmem_limit_bytes=grant * 2**20),
    )(*args)


def power_of(top):
    return jnp.floor(jnp.log2(jnp.maximum(top, 1e-30))) + 1.0


def encode_heads(parts, code_ref):
    rows = parts[0].shape[0]
    lane = lax.broadcasted_iota(I32, (rows, LANES), 1)
    tops = jnp.zeros((rows, LANES), F32)
    for h, part in enumerate(parts):
        tops = jnp.where(lane == h, jnp.max(jnp.abs(part), axis=1, keepdims=True), tops)
    power = power_of(tops)
    scale = jnp.exp2(-power) * CODE_TOP
    for h, part in enumerate(parts):
        code = jnp.round(part * scale[:, h : h + 1])
        code_ref[h * rows : (h + 1) * rows, :] = code.astype(I32).astype(I16)
    square = jnp.concatenate([power, jnp.zeros((LANES - rows, LANES), F32)], axis=0)
    code_ref[len(parts) * rows :, :] = jnp.transpose(square)[:TAIL].astype(I32).astype(I16)


def scales_of(code_ref, rows):
    lines = code_ref[code_ref.shape[0] - TAIL :, :].astype(I32).astype(F32)
    square = jnp.concatenate([lines, jnp.zeros((LANES - TAIL, LANES), F32)], axis=0)
    return jnp.exp2(jnp.transpose(square)[:rows]) * (1.0 / CODE_TOP)


def decode_head(code_ref, scales, h):
    rows = scales.shape[0]
    return code_ref[h * rows : (h + 1) * rows, :].astype(I32).astype(F32) * scales[:, h : h + 1]


def begin_kernel(ds, x_hbm, w_hbm, key_hbm, value_hbm, mask_hbm, *rest):
    groups = len(ds)
    first, other, packs = rest[:2], rest[2:4], rest[4 : 4 + groups]
    x_ref, w_buf, key_ref, value_ref, mask_ref, sems = rest[4 + groups :]
    half = x_ref.shape[0] // 2
    width = w_buf.shape[2]
    keys = key_ref.shape[0]

    def fetch(source, target, n):
        copy = pltpu.make_async_copy(source, target, sems.at[n])
        copy.start()
        return copy

    def weights(i):
        at = pl.multiple_of((ids[2] ^ ds[i]) * width, width)
        return fetch(w_hbm.at[:, pl.ds(at, width)], w_buf.at[i], i)

    text = fetch(x_hbm, x_ref, groups)
    copies = [weights(0)]
    tokens = [fetch(key_hbm, key_ref, groups + 1), fetch(value_hbm, value_ref, groups + 2)]
    tokens.append(fetch(mask_hbm, mask_ref, groups + 3))
    copies += [weights(i) for i in range(1, groups)]
    peer = pl.multiple_of((1 - ids[0]) * half, half)
    mine = pl.multiple_of(ids[0] * half, half)

    def project(i, send_ref, keep_ref, at):
        copies[i].wait()
        cols = slice(at * width, (at + 1) * width)
        w = w_buf[i]
        send_ref[:, cols] = jnp.dot(x_ref[pl.ds(peer, half), :], w, preferred_element_type=F32)
        keep_ref[:, cols] = jnp.dot(x_ref[pl.ds(mine, half), :], w, preferred_element_type=F32)

    text.wait()
    project(0, *first, 0)
    for copy in tokens:
        copy.wait()
    line = lax.broadcasted_iota(I32, (TAIL, LANES), 0)
    tail = jnp.zeros((TAIL, LANES), F32)
    segments, text_rows = mask_ref.shape
    for s in range(segments):
        for j in range(text_rows // LANES):
            row = mask_ref[s : s + 1, j * LANES : (j + 1) * LANES]
            here = line == s * (text_rows // LANES) + j
            tail = jnp.where(here & (row == 1), F32(1.0), tail)
    for d in range(groups):
        at = pl.multiple_of((ids[2] ^ d) * LANES, LANES)
        packs[d][:keys, :] = key_ref[:, pl.ds(at, LANES)]
        for c in range(keys // LANES):
            block = value_ref[c * LANES : (c + 1) * LANES, pl.ds(at, LANES)]
            packs[d][keys + c * LANES : keys + (c + 1) * LANES, :] = jnp.transpose(block)
        packs[d][2 * keys :, :] = tail.astype(BF16)
    for i in range(1, groups):
        project(i, *other, i - 1)


def split_x_kernel(first, keep_ref, got_ref, code_ref, own_ref):
    half, width = own_ref.shape
    first *= width
    mine = pl.multiple_of(ids[1] * half, half)
    peer = pl.multiple_of((1 - ids[1]) * half, half)
    parts = []
    for h in range(width // LANES):
        cols = slice(first + h * LANES, first + (h + 1) * LANES)
        parts.append(keep_ref[pl.ds(peer, half), cols] + got_ref[pl.ds(peer, half), cols])
    encode_heads(parts, code_ref)
    cols = slice(first, first + width)
    own_ref[...] = keep_ref[pl.ds(mine, half), cols] + got_ref[pl.ds(mine, half), cols]


def split_z_kernel(ds, own_ref, got_ref, *outs):
    heads = own_ref.shape[1] // len(ds) // LANES
    scales = scales_of(got_ref, own_ref.shape[0])
    for i, d in enumerate(ds):
        parts = []
        for h in range(i * heads, (i + 1) * heads):
            parts.append(own_ref[:, h * LANES : (h + 1) * LANES] + decode_head(got_ref, scales, h))
        if d:
            encode_heads(parts, outs[i])
        else:
            for h, part in enumerate(parts):
                outs[i][:, h * LANES : (h + 1) * LANES] = part


def norm_kernel(own_ref, gain_ref, *rest):
    got, out_ref = rest[:-1], rest[-1]
    gain = gain_ref[...]
    scales = [scales_of(g, own_ref.shape[0]) for g in got]
    for h in range(out_ref.shape[1] // LANES):
        cols = slice(h * LANES, (h + 1) * LANES)
        total = own_ref[:, cols]
        for g, scale in zip(got, scales):
            total = total + decode_head(g, scale, h)
        mean_sq = jnp.mean(total * total, axis=1, keepdims=True)
        out_ref[:, cols] = (total * lax.rsqrt(mean_sq + 1e-05) * gain).astype(BF16)


def attend_kernel(ds, heads, segments, rel, begin, finish, q_ref, lens_ref, *rest):
    packs, rest = rest[: len(ds)], rest[len(ds) :]
    state, outs = (None, rest) if begin else (rest[:2], rest[2:])
    rows = q_ref.shape[0]
    keys = (packs[0].shape[0] - TAIL) // 2
    seg = keys // segments
    units = heads * rows // LANES
    scale = 1.4426950408889634 / LANES**0.5
    core, x = ids[0] ^ (rel & 1), ids[1] ^ (rel >> 1)
    low_lanes = lax.broadcasted_iota(I32, (8, LANES), 1) < rows
    take_low = jnp.full((8, LANES), 1 - x, I32) == 1

    def twice(row):
        wide = jnp.broadcast_to(row, (8, LANES))
        turned = pltpu.roll(wide, rows, 1)
        return jnp.where(take_low == low_lanes, wide, turned)[:1]

    lens = twice(jnp.where(core == 1, lens_ref[1:2, :], lens_ref[0:1, :]))
    stacked = jnp.concatenate([q_ref[:, h * LANES : (h + 1) * LANES] for h in range(heads)], axis=0)
    highs, sums, nums = [], [], []
    for b, pack in zip(ds, packs):
        raw = lax.dot_general(pack[:keys, :], stacked, (((1,), (1,)), ((), ())), preferred_element_type=F32)
        tail = pack[2 * keys :, :].astype(F32)
        first = ((ids[2] ^ b) * 4 + ids[1] * 2 + ids[0]) * keys
        masks = []
        for s in range(segments):
            seen = twice(jnp.where(core == 1, tail[2 * s + 1 : 2 * s + 2, :], tail[2 * s : 2 * s + 1, :]))
            limit = jnp.where(seen > 0.5, lens - (first + s * seg), 0)
            inside = lax.broadcasted_iota(I32, (seg, LANES), 0) < limit
            masks.append(jnp.where(inside, F32(0.0), F32(LOW)))
        bias = jnp.concatenate(masks, axis=0)
        unit_highs, unit_sums, unit_weights = [], [], []
        for u in range(units):
            scores = raw[:, u * LANES : (u + 1) * LANES] * scale + bias
            high = jnp.maximum(jnp.max(scores, axis=0, keepdims=True), -1e29)
            weights = jnp.exp2(scores - high)
            unit_highs.append(high)
            unit_sums.append(jnp.sum(weights, axis=0, keepdims=True))
            unit_weights.append(weights.astype(BF16))
        highs.append(jnp.concatenate(unit_highs, axis=1))
        sums.append(jnp.concatenate(unit_sums, axis=1))
        value = jnp.concatenate(
            [pack[keys + c * LANES : keys + (c + 1) * LANES, :] for c in range(keys // LANES)], axis=1
        )
        nums.append(jnp.dot(value, jnp.concatenate(unit_weights, axis=1), preferred_element_type=F32))
    if not begin:
        highs.append(state[1][:1, :])
        sums.append(state[1][1:2, :])
        nums.append(state[0][...])
    top = functools.reduce(jnp.maximum, highs)
    factors = [jnp.exp2(h - top) for h in highs]
    total = functools.reduce(jnp.add, [s * f for s, f in zip(sums, factors)])
    num = functools.reduce(jnp.add, [n * f for n, f in zip(nums, factors)])
    if not finish:
        outs[0][...] = num
        line = lax.broadcasted_iota(I32, outs[1].shape, 0)
        outs[1][...] = jnp.where(line == 0, top, total)
        return
    some = total > 0.0
    out = num * jnp.where(some, 1.0 / jnp.where(some, total, 1.0), 0.0)
    level = jnp.where(some, top + jnp.log2(jnp.where(some, total, 1.0)), NO_SUM)
    if rel == 0:
        out_ref, level_ref = outs
        out_ref[...] = out
        level_ref[...] = jnp.broadcast_to(level, level_ref.shape)
        return
    (code_ref,) = outs
    power = power_of(jnp.max(jnp.abs(out), axis=0, keepdims=True))
    code_ref[:LANES, :] = jnp.round(out * (jnp.exp2(-power) * CODE_TOP)).astype(I32).astype(I16)
    whole = jnp.round(level)
    fine = jnp.clip(jnp.round((level - whole) * 65536.0), -32767.0, 32767.0)
    line = lax.broadcasted_iota(I32, (TAIL, heads * rows), 0)
    tail = jnp.where(line == 0, power, jnp.where(line == 1, whole, jnp.where(line == 2, fine, 0.0)))
    code_ref[LANES:, :] = tail.astype(I32).astype(I16)


def merge_kernel(heads, own_ref, level_ref, *rest):
    got, out_ref = rest[:-1], rest[-1]
    rows = out_ref.shape[0]
    tails = [g[LANES:, :].astype(I32).astype(F32) for g in got]
    levels = [level_ref[:1, :]] + [t[1:2] + t[2:3] * (1.0 / 65536.0) for t in tails]
    top = functools.reduce(jnp.maximum, levels)
    shares = [jnp.exp2(level - top) for level in levels]
    inverse = 1.0 / functools.reduce(jnp.add, shares)
    num = own_ref[...] * (shares[0] * inverse)
    for g, tail, share in zip(got, tails, shares[1:]):
        weight = jnp.exp2(tail[:1]) * (1.0 / CODE_TOP) * share * inverse
        num = num + g[:LANES, :].astype(I32).astype(F32) * weight
    per = LANES // rows
    for u in range(heads // per):
        block = jnp.transpose(num[:, u * LANES : (u + 1) * LANES])
        for p in range(per):
            h = u * per + p
            out_ref[:, h * LANES : (h + 1) * LANES] = block[p * rows : (p + 1) * rows].astype(BF16)


def output_part(ds, blocks, w_ref):
    width = blocks[0][0].shape[1]
    groups = w_ref.shape[0] // width
    total = None
    for d, row_blocks in zip(ds, blocks):
        left = jnp.concatenate([b[...] for b in row_blocks], axis=0)
        base = pl.multiple_of(lax.rem(ids[2] + groups - d, groups) * width, width)
        part = jnp.dot(left, w_ref[pl.ds(base, width), :], preferred_element_type=F32)
        total = part if total is None else total + part
    return total


def output_kernel(ds, begin, finish, w_ref, *rest):
    count = 2 * len(ds)
    blocks = [rest[2 * i : 2 * i + 2] for i in range(len(ds))]
    rest = rest[count:]
    total = output_part(ds, blocks, w_ref)
    if not begin:
        total = total + rest[0][...]
        rest = rest[1:]
    if not finish:
        rest[0][...] = total
        return
    keep_ref, code_ref = rest
    rows, width = keep_ref.shape
    own, other = total[:rows], total[rows:]
    keep_own = jnp.full((rows, 1), (ids[0] == ids[3]).astype(I32), I32) == 1
    keep_ref[...] = jnp.where(keep_own, own, other)
    send = jnp.where(keep_own, other, own)
    power = power_of(jnp.max(jnp.abs(send), axis=0, keepdims=True))
    code_ref[:rows, :] = jnp.round(send * (jnp.exp2(-power) * CODE_TOP)).astype(I32).astype(I16)
    code_ref[rows:, :] = jnp.broadcast_to(power, (TAIL, width)).astype(I32).astype(I16)


def finish_kernel(keep_near, got_near, keep_far, got_far, text_ref, out_ref):
    half = out_ref.shape[0]
    rows = half // 2
    for far, (keep_ref, got_ref) in enumerate(((keep_near, got_near), (keep_far, got_far))):
        at = pl.multiple_of((ids[1] ^ far) * rows, rows)
        scale = jnp.exp2(got_ref[rows:, :].astype(I32).astype(F32)[:1]) * (1.0 / CODE_TOP)
        total = keep_ref[...] + got_ref[:rows, :].astype(I32).astype(F32) * scale
        text = text_ref[pl.ds(pl.multiple_of(ids[3] * half + at, rows), rows), :]
        out_ref[pl.ds(at, rows), :] = (text.astype(F32) + total).astype(BF16)


def fast_shards(text_states, q_weight, q_gain, key_cache, value_cache, block_mask, lengths, o_weight):
    ctx = lax.axis_size("ctx")
    struct = jax.ShapeDtypeStruct
    text_rows, depth = text_states.shape
    columns = q_weight.shape[1]
    keys = key_cache.shape[0]
    groups = key_cache.shape[1] // LANES
    width = columns // groups
    heads = width // LANES
    rows, half = text_rows // 4, text_rows // 2
    pairs = heads * rows
    segments = block_mask.shape[1]
    out_cols = o_weight.shape[1]

    def swap(value, bits):
        return lax.ppermute(value, "ctx", [(i, i ^ bits) for i in range(ctx)])

    def turn(value, shift):
        return lax.ppermute(value, "ctx", [(i, (i + shift) % ctx) for i in range(ctx)])

    def after(value, *others):
        return lax.optimization_barrier((value, *others))[0]

    in_hbm = functools.partial(pltpu.with_memory_space_constraint, memory_space=pltpu.HBM)
    order = list(range(groups - 1, -1, -1))
    chunks = [groups - 1, *[d for d in range(1, groups - 1)], 0]
    parts = [struct((half, width), F32)] * 2 + [struct((half, (groups - 1) * width), F32)] * 2
    sent, kept, sent_more, kept_more, *packs = call(
        functools.partial(begin_kernel, chunks),
        (*parts, *[struct((2 * keys + TAIL, LANES), BF16)] * groups),
        (in_hbm(text_states), in_hbm(q_weight), in_hbm(key_cache), in_hbm(value_cache), in_hbm(block_mask.T)),
        flops=2 * text_rows * depth * columns,
        specs=[HB] * 5,
        scratch=[
            pltpu.VMEM(text_states.shape, BF16),
            pltpu.VMEM((groups, depth, width), BF16),
            pltpu.VMEM(key_cache.shape, BF16),
            pltpu.VMEM(value_cache.shape, BF16),
            pltpu.VMEM((segments, text_rows), I32),
            pltpu.SemaphoreType.DMA((groups + 4,)),
        ],
    )
    packs = [packs[0]] + [swap(packs[d], 4 * d) for d in range(1, groups)]
    halves = (kept, swap(sent, 1))
    more = (kept_more, swap(sent_more, 1))

    sums = {}
    for n, d in enumerate(chunks):
        code, own = call(
            functools.partial(split_x_kernel, max(n - 1, 0)),
            (struct((pairs + TAIL, LANES), I16), struct((rows, width), F32)),
            more if n else halves,
        )
        got = swap(code, 2)
        (out,) = call(
            functools.partial(split_z_kernel, [d]),
            (struct((pairs + TAIL, LANES), I16) if d else struct((rows, width), F32),),
            (own, got),
        )
        sums[d] = swap(out, 4 * d) if d else out
    normed = call(
        norm_kernel,
        struct((rows, width), BF16),
        (sums[0], q_gain.reshape(1, LANES), *[sums[d] for d in range(1, groups)]),
    )

    lens = lengths.reshape(2, LANES)
    last = groups // 2
    first = [d for d in order[::-1] if d != last]
    queries = {t: swap(normed, t) if t else normed for t in range(4)}
    states, previous = {}, ()
    for rel in range(4):
        states[rel] = call(
            functools.partial(attend_kernel, first, heads, segments, rel, True, False),
            (struct((LANES, pairs), F32), struct((8, pairs), F32)),
            (after(queries[rel], *previous), lens, *[packs[d] for d in first]),
            flops=4 * pairs * keys * len(first) * LANES,
        )
        previous = states[rel]
    outs = {}
    for rel in (2, 3, 1, 0):
        if rel:
            shape = struct((LANES + TAIL, pairs), I16)
        else:
            shape = (struct((LANES, pairs), F32), struct((8, pairs), F32))
        res = call(
            functools.partial(attend_kernel, [last], heads, segments, rel, False, True),
            shape,
            (after(queries[rel], previous), lens, packs[last], *states[rel]),
            flops=4 * pairs * keys * LANES,
        )
        previous = res
        outs[rel] = swap(res, rel) if rel else res
    attended = call(
        functools.partial(merge_kernel, heads),
        struct((rows, width), BF16),
        (*outs[0], outs[1], outs[2], outs[3]),
    )

    column = {d: turn(attended, 4 * d) if d else attended for d in order}
    beside = {d: swap(column[d], 2) for d in range(groups)}
    early, late = list(range(groups // 2)), list(range(groups // 2, groups))
    tail_d = late[0]

    def over_core(values):
        if len(values) == 1:
            return [swap(values[0], 1)]
        moved = swap(jnp.stack(values), 1)
        return [moved[i] for i in range(len(values))]

    blocks = {}
    moved = over_core([b for d in early for b in (column[d], beside[d])])
    for i, d in enumerate(early):
        blocks[d] = (column[d], beside[d], moved[2 * i], moved[2 * i + 1])
    pairs_late = [(d, side) for d in reversed(late) for side in (column, beside)][:-1]
    moved = over_core([side[d] for d, side in pairs_late])
    end = over_core([beside[tail_d]])
    moved = moved + end
    for i, d in enumerate(reversed(late)):
        blocks[d] = (column[d], beside[d], moved[2 * i], moved[2 * i + 1])
    near = {d: (blocks[d][0], blocks[d][2]) for d in range(groups)}
    far = {d: (blocks[d][1], blocks[d][3]) for d in range(groups)}

    def output(ds, rows_of, begin, finish, *before):
        done = (struct((rows, out_cols), F32), struct((rows + TAIL, out_cols), I16))
        return call(
            functools.partial(output_kernel, ds, begin, finish),
            done if finish else struct((2 * rows, out_cols), F32),
            (o_weight, *[b for d in ds for b in rows_of[d]], *before),
            flops=4 * rows * width * len(ds) * out_cols,
        )

    def trade(code):
        return lax.ppermute(code, ("head", "tp"), [(0, 1), (1, 0)])

    before = output([d for d in range(groups) if d != tail_d], far, True, False)
    keep_near, code = output(list(range(groups)), near, True, True)
    got_near = trade(code)
    keep_far, code = output([tail_d], far, False, True, before)
    got_far = trade(code)
    return call(
        finish_kernel,
        struct((half, out_cols), BF16),
        (keep_near, got_near, keep_far, got_far, text_states),
    )


def plain_shards(
    text_states,
    q_weight,
    q_gain,
    visual_key_cache,
    visual_value_cache,
    block_mask,
    lengths,
    o_weight,
):
    text_rows = text_states.shape[0]
    columns = q_weight.shape[1]
    head_dim = q_gain.shape[0]
    query_heads = columns // head_dim
    kv_heads = visual_key_cache.shape[1] // head_dim
    query_group_count = query_heads // kv_heads
    row_block = text_states
    query_share = lax.psum_scatter(
        jnp.dot(row_block, q_weight, preferred_element_type=jnp.float32),
        "ctx",
        scatter_dimension=0,
        tiled=True,
    )
    shaped = query_share.reshape(query_share.shape[0], query_heads, head_dim)
    mean_sq = jnp.mean(shaped * shaped, axis=-1, keepdims=True)
    normed = shaped * lax.rsqrt(mean_sq + 1e-05) * q_gain
    queries = lax.all_gather(
        normed.reshape(query_share.shape[0], columns).astype(jnp.bfloat16),
        "ctx",
        axis=0,
        tiled=True,
    )
    keys_local = visual_key_cache.shape[0]
    segment_len = keys_local // block_mask.shape[1]
    key_block_offset = lax.axis_index("ctx") * keys_local
    positions = key_block_offset + jnp.arange(keys_local, dtype=jnp.int32)
    allowed = (jnp.repeat(block_mask, segment_len, axis=1) == 1) & (
        positions[None, :] < lengths[:, None]
    )
    score_scale = 1.0 / head_dim**0.5
    partial_nums = []
    partial_maxes = []
    partial_totals = []
    for q_head in range(query_heads):
        kv_head = q_head // query_group_count
        query_part = queries[:, q_head * head_dim : (q_head + 1) * head_dim]
        key_part = visual_key_cache[:, kv_head * head_dim : (kv_head + 1) * head_dim]
        value_part = visual_value_cache[:, kv_head * head_dim : (kv_head + 1) * head_dim]
        scores = (
            lax.dot_general(
                query_part, key_part, (((1,), (1,)), ((), ())), preferred_element_type=jnp.float32
            )
            * score_scale
        )
        scores = jnp.where(allowed, scores, jnp.float32(-1e30))
        local_max = jnp.max(scores, axis=1)
        weights = jnp.where(allowed, jnp.exp(scores - local_max[:, None]), jnp.float32(0.0))
        partial_totals.append(jnp.sum(weights, axis=1))
        partial_maxes.append(local_max)
        partial_nums.append(
            jnp.dot(weights.astype(jnp.bfloat16), value_part, preferred_element_type=jnp.float32)
        )
    local_num = jnp.concatenate(partial_nums, axis=1)
    local_max = jnp.stack(partial_maxes, axis=1)
    local_total = jnp.stack(partial_totals, axis=1)
    highest = lax.pmax(local_max, "ctx")
    factor = jnp.exp(local_max - highest)
    scaled_num = local_num * jnp.repeat(factor, head_dim, axis=1)
    scaled_total = local_total * factor
    owned_num, owned_total = (
        lax.psum_scatter(scaled_num, "ctx", scatter_dimension=0, tiled=True),
        lax.psum_scatter(scaled_total, "ctx", scatter_dimension=0, tiled=True),
    )
    owned = (owned_num / jnp.repeat(owned_total, head_dim, axis=1)).astype(jnp.bfloat16)
    attended = lax.all_gather(owned, "ctx", axis=0, tiled=True)
    rows_out = text_rows // lax.axis_size(("head", "tp"))
    row_block = attended
    summed = lax.psum_scatter(
        jnp.dot(row_block, o_weight, preferred_element_type=jnp.float32),
        ("head", "tp"),
        scatter_dimension=0,
        tiled=True,
    )
    residual = lax.dynamic_slice_in_dim(
        text_states, lax.axis_index(("head", "tp")) * rows_out, rows_out, 0
    )
    return (residual.astype(jnp.float32) + summed).astype(jnp.bfloat16)


def solution(mesh):
    in_specs = (
        P(None, "ctx"),
        P("ctx", ("head", "tp")),
        P(),
        P("ctx", ("head", "tp")),
        P("ctx", ("head", "tp")),
        P(None, "ctx"),
        P(),
        P(("head", "tp"), "ctx"),
    )
    out_specs = P(("head", "tp"), "ctx")
    ctx, halves = mesh.shape["ctx"], mesh.shape["head"] * mesh.shape["tp"]

    def fits(args):
        text_rows = args[0].shape[0]
        groups = args[3].shape[1] // args[2].shape[0]
        return (
            args[2].shape[0] == LANES
            and halves == 2
            and text_rows == 2 * LANES
            and groups == 4
            and ctx == 4 * groups
            and args[1].shape[1] % (groups * LANES) == 0
            and args[1].shape[1] // groups <= LANES * LANES
            and 2 * args[5].shape[1] <= TAIL
            and args[3].shape[0] % (args[5].shape[1] * LANES) == 0
        )

    def shards(*args):
        if not fits(args):
            return plain_shards(*args)
        return fast_shards(*args)

    spread = jax.shard_map(shards, mesh=mesh, in_specs=in_specs, out_specs=out_specs, check_vma=False)
    if halves != 2 or ctx != 16:
        return spread
    return spread
```

```python
import functools

import jax
import jax.numpy as jnp
from jax import lax
from jax.experimental import pallas as pl
from jax.experimental.pallas import tpu as pltpu
from jax.sharding import PartitionSpec as P


F32, BF16, I16, I32 = jnp.float32, jnp.bfloat16, jnp.int16, jnp.int32
LANES = 128
TAIL = 16
CODE_TOP = 32000.0
LOW = -1e30
NO_SUM = -32000.0
VM = pl.BlockSpec(memory_space=pltpu.VMEM)
HB = pl.BlockSpec(memory_space=pltpu.HBM)


class Position:
    def __getitem__(self, i):
        me = lax.axis_index("ctx")
        if i == 0:
            return lax.rem(me, 2)
        if i == 1:
            return lax.rem(lax.div(me, 2), 2)
        if i == 2:
            return lax.div(me, 4)
        return lax.axis_index("head") * lax.axis_size("tp") + lax.axis_index("tp")


ids = Position()


def call(kernel, out_shape, args, flops=0, specs=None, scratch=(), grant=16):
    moved = sum(a.size * a.dtype.itemsize for a in args)
    moved += sum(o.size * o.dtype.itemsize for o in jax.tree.leaves(out_shape))
    return pl.pallas_call(
        kernel,
        out_shape=out_shape,
        in_specs=specs or [VM] * len(args),
        out_specs=jax.tree.map(lambda _: VM, out_shape),
        scratch_shapes=list(scratch),
        cost_estimate=pl.CostEstimate(flops=int(flops), bytes_accessed=int(moved), transcendentals=0),
        compiler_params=pltpu.CompilerParams(vmem_limit_bytes=grant * 2**20),
    )(*args)


def power_of(top):
    return jnp.floor(jnp.log2(jnp.maximum(top, 1e-30))) + 1.0


def encode_heads(parts, code_ref):
    rows = parts[0].shape[0]
    lane = lax.broadcasted_iota(I32, (rows, LANES), 1)
    tops = jnp.zeros((rows, LANES), F32)
    for h, part in enumerate(parts):
        tops = jnp.where(lane == h, jnp.max(jnp.abs(part), axis=1, keepdims=True), tops)
    power = power_of(tops)
    scale = jnp.exp2(-power) * CODE_TOP
    for h, part in enumerate(parts):
        code = jnp.round(part * scale[:, h : h + 1])
        code_ref[h * rows : (h + 1) * rows, :] = code.astype(I32).astype(I16)
    square = jnp.concatenate([power, jnp.zeros((LANES - rows, LANES), F32)], axis=0)
    code_ref[len(parts) * rows :, :] = jnp.transpose(square)[:TAIL].astype(I32).astype(I16)


def scales_of(code_ref, rows):
    lines = code_ref[code_ref.shape[0] - TAIL :, :].astype(I32).astype(F32)
    square = jnp.concatenate([lines, jnp.zeros((LANES - TAIL, LANES), F32)], axis=0)
    return jnp.exp2(jnp.transpose(square)[:rows]) * (1.0 / CODE_TOP)


def decode_head(code_ref, scales, h):
    rows = scales.shape[0]
    return code_ref[h * rows : (h + 1) * rows, :].astype(I32).astype(F32) * scales[:, h : h + 1]


def pack_kernel(key_hbm, value_hbm, mask_hbm, *rest):
    packs, (key_ref, value_ref, mask_ref, sems) = rest[:-4], rest[-4:]
    keys = key_ref.shape[0]
    copies = []
    for n, (source, target) in enumerate(((value_hbm, value_ref), (key_hbm, key_ref), (mask_hbm, mask_ref))):
        copies.append(pltpu.make_async_copy(source, target, sems.at[n]))
        copies[-1].start()
    for copy in copies:
        copy.wait()
    line = lax.broadcasted_iota(I32, (TAIL, LANES), 0)
    tail = jnp.zeros((TAIL, LANES), F32)
    segments, text_rows = mask_ref.shape
    for s in range(segments):
        for j in range(text_rows // LANES):
            row = mask_ref[s : s + 1, j * LANES : (j + 1) * LANES]
            here = line == s * (text_rows // LANES) + j
            tail = jnp.where(here & (row == 1), F32(1.0), tail)
    for d in range(len(packs)):
        at = pl.multiple_of((ids[2] ^ d) * LANES, LANES)
        packs[d][:keys, :] = key_ref[:, pl.ds(at, LANES)]
        for c in range(keys // LANES):
            block = value_ref[c * LANES : (c + 1) * LANES, pl.ds(at, LANES)]
            packs[d][keys + c * LANES : keys + (c + 1) * LANES, :] = jnp.transpose(block)
        packs[d][2 * keys :, :] = tail.astype(BF16)


def project_kernel(ds, x_hbm, w_hbm, send_ref, keep_ref, more_ref, kept_ref, x_ref, w_buf, sems):
    half = x_ref.shape[0] // 2
    width = w_buf.shape[2]
    text = pltpu.make_async_copy(x_hbm, x_ref, sems.at[len(ds)])
    text.start()
    copies = []
    for i, d in enumerate(ds):
        at = pl.multiple_of((ids[2] ^ d) * width, width)
        copies.append(pltpu.make_async_copy(w_hbm.at[:, pl.ds(at, width)], w_buf.at[i], sems.at[i]))
        copies[-1].start()
    peer = pl.multiple_of((1 - ids[0]) * half, half)
    mine = pl.multiple_of(ids[0] * half, half)
    text.wait()
    for i in range(len(ds)):
        copies[i].wait()
        send, keep, at = (send_ref, keep_ref, 0) if i == 0 else (more_ref, kept_ref, i - 1)
        cols = slice(at * width, (at + 1) * width)
        w = w_buf[i]
        send[:, cols] = jnp.dot(x_ref[pl.ds(peer, half), :], w, preferred_element_type=F32)
        keep[:, cols] = jnp.dot(x_ref[pl.ds(mine, half), :], w, preferred_element_type=F32)


def split_x_kernel(first, keep_ref, got_ref, code_ref, own_ref):
    half, width = own_ref.shape
    first *= width
    mine = pl.multiple_of(ids[1] * half, half)
    peer = pl.multiple_of((1 - ids[1]) * half, half)
    parts = []
    for h in range(width // LANES):
        cols = slice(first + h * LANES, first + (h + 1) * LANES)
        parts.append(keep_ref[pl.ds(peer, half), cols] + got_ref[pl.ds(peer, half), cols])
    encode_heads(parts, code_ref)
    cols = slice(first, first + width)
    own_ref[...] = keep_ref[pl.ds(mine, half), cols] + got_ref[pl.ds(mine, half), cols]


def split_z_kernel(ds, own_ref, got_ref, *outs):
    heads = own_ref.shape[1] // len(ds) // LANES
    scales = scales_of(got_ref, own_ref.shape[0])
    for i, d in enumerate(ds):
        parts = []
        for h in range(i * heads, (i + 1) * heads):
            parts.append(own_ref[:, h * LANES : (h + 1) * LANES] + decode_head(got_ref, scales, h))
        if d:
            encode_heads(parts, outs[i])
        else:
            for h, part in enumerate(parts):
                outs[i][:, h * LANES : (h + 1) * LANES] = part


def norm_kernel(own_ref, gain_ref, *rest):
    got, out_ref = rest[:-1], rest[-1]
    gain = gain_ref[...]
    scales = [scales_of(g, own_ref.shape[0]) for g in got]
    for h in range(out_ref.shape[1] // LANES):
        cols = slice(h * LANES, (h + 1) * LANES)
        total = own_ref[:, cols]
        for g, scale in zip(got, scales):
            total = total + decode_head(g, scale, h)
        mean_sq = jnp.mean(total * total, axis=1, keepdims=True)
        out_ref[:, cols] = (total * lax.rsqrt(mean_sq + 1e-05) * gain).astype(BF16)


def attend_kernel(ds, heads, segments, rel, begin, finish, q_ref, lens_ref, *rest):
    packs, rest = rest[: len(ds)], rest[len(ds) :]
    state, outs = (None, rest) if begin else (rest[:2], rest[2:])
    rows = q_ref.shape[0]
    keys = (packs[0].shape[0] - TAIL) // 2
    seg = keys // segments
    units = heads * rows // LANES
    scale = 1.4426950408889634 / LANES**0.5
    core, x = ids[0] ^ (rel & 1), ids[1] ^ (rel >> 1)
    low_lanes = lax.broadcasted_iota(I32, (8, LANES), 1) < rows
    take_low = jnp.full((8, LANES), 1 - x, I32) == 1

    def twice(row):
        wide = jnp.broadcast_to(row, (8, LANES))
        turned = pltpu.roll(wide, rows, 1)
        return jnp.where(take_low == low_lanes, wide, turned)[:1]

    lens = twice(jnp.where(core == 1, lens_ref[1:2, :], lens_ref[0:1, :]))
    stacked = jnp.concatenate([q_ref[:, h * LANES : (h + 1) * LANES] for h in range(heads)], axis=0)
    highs, sums, nums = [], [], []
    for b, pack in zip(ds, packs):
        raw = lax.dot_general(pack[:keys, :], stacked, (((1,), (1,)), ((), ())), preferred_element_type=F32)
        tail = pack[2 * keys :, :].astype(F32)
        first = ((ids[2] ^ b) * 4 + ids[1] * 2 + ids[0]) * keys
        masks = []
        for s in range(segments):
            seen = twice(jnp.where(core == 1, tail[2 * s + 1 : 2 * s + 2, :], tail[2 * s : 2 * s + 1, :]))
            limit = jnp.where(seen > 0.5, lens - (first + s * seg), 0)
            inside = lax.broadcasted_iota(I32, (seg, LANES), 0) < limit
            masks.append(jnp.where(inside, F32(0.0), F32(LOW)))
        bias = jnp.concatenate(masks, axis=0)
        unit_highs, unit_sums, unit_weights = [], [], []
        for u in range(units):
            scores = raw[:, u * LANES : (u + 1) * LANES] * scale + bias
            high = jnp.maximum(jnp.max(scores, axis=0, keepdims=True), -1e29)
            weights = jnp.exp2(scores - high)
            unit_highs.append(high)
            unit_sums.append(jnp.sum(weights, axis=0, keepdims=True))
            unit_weights.append(weights.astype(BF16))
        highs.append(jnp.concatenate(unit_highs, axis=1))
        sums.append(jnp.concatenate(unit_sums, axis=1))
        value = jnp.concatenate(
            [pack[keys + c * LANES : keys + (c + 1) * LANES, :] for c in range(keys // LANES)], axis=1
        )
        nums.append(jnp.dot(value, jnp.concatenate(unit_weights, axis=1), preferred_element_type=F32))
    if not begin:
        highs.append(state[1][:1, :])
        sums.append(state[1][1:2, :])
        nums.append(state[0][...])
    top = functools.reduce(jnp.maximum, highs)
    factors = [jnp.exp2(h - top) for h in highs]
    total = functools.reduce(jnp.add, [s * f for s, f in zip(sums, factors)])
    num = functools.reduce(jnp.add, [n * f for n, f in zip(nums, factors)])
    if not finish:
        outs[0][...] = num
        line = lax.broadcasted_iota(I32, outs[1].shape, 0)
        outs[1][...] = jnp.where(line == 0, top, total)
        return
    some = total > 0.0
    out = num * jnp.where(some, 1.0 / jnp.where(some, total, 1.0), 0.0)
    level = jnp.where(some, top + jnp.log2(jnp.where(some, total, 1.0)), NO_SUM)
    if rel == 0:
        out_ref, level_ref = outs
        out_ref[...] = out
        level_ref[...] = jnp.broadcast_to(level, level_ref.shape)
        return
    (code_ref,) = outs
    power = power_of(jnp.max(jnp.abs(out), axis=0, keepdims=True))
    code_ref[:LANES, :] = jnp.round(out * (jnp.exp2(-power) * CODE_TOP)).astype(I32).astype(I16)
    whole = jnp.round(level)
    fine = jnp.clip(jnp.round((level - whole) * 65536.0), -32767.0, 32767.0)
    line = lax.broadcasted_iota(I32, (TAIL, heads * rows), 0)
    tail = jnp.where(line == 0, power, jnp.where(line == 1, whole, jnp.where(line == 2, fine, 0.0)))
    code_ref[LANES:, :] = tail.astype(I32).astype(I16)


def merge_kernel(heads, own_ref, level_ref, *rest):
    got, out_ref = rest[:-1], rest[-1]
    rows = out_ref.shape[0]
    tails = [g[LANES:, :].astype(I32).astype(F32) for g in got]
    levels = [level_ref[:1, :]] + [t[1:2] + t[2:3] * (1.0 / 65536.0) for t in tails]
    top = functools.reduce(jnp.maximum, levels)
    shares = [jnp.exp2(level - top) for level in levels]
    inverse = 1.0 / functools.reduce(jnp.add, shares)
    num = own_ref[...] * (shares[0] * inverse)
    for g, tail, share in zip(got, tails, shares[1:]):
        weight = jnp.exp2(tail[:1]) * (1.0 / CODE_TOP) * share * inverse
        num = num + g[:LANES, :].astype(I32).astype(F32) * weight
    per = LANES // rows
    for u in range(heads // per):
        block = jnp.transpose(num[:, u * LANES : (u + 1) * LANES])
        for p in range(per):
            h = u * per + p
            out_ref[:, h * LANES : (h + 1) * LANES] = block[p * rows : (p + 1) * rows].astype(BF16)


def output_rows_kernel(ds, tail_d, w_ref, *rest):
    blocks, (near_ref, far_ref) = rest[:-2], rest[-2:]
    rows, width = blocks[0].shape
    groups = w_ref.shape[0] // width
    near = far = None
    blocks = list(blocks)
    for d in ds:
        base = pl.multiple_of(lax.rem(ids[2] + groups - d, groups) * width, width)
        w = w_ref[pl.ds(base, width), :]
        if d == tail_d:
            part = jnp.dot(blocks.pop(0)[...], w, preferred_element_type=F32)
        else:
            left = jnp.concatenate([blocks.pop(0)[...], blocks.pop(0)[...]], axis=0)
            part = jnp.dot(left, w, preferred_element_type=F32)
            far = part[rows:] if far is None else far + part[rows:]
        near = part[:rows] if near is None else near + part[:rows]
    near_ref[...] = near
    far_ref[...] = far


def split_rows(own, other, keep_ref, code_ref):
    rows, width = keep_ref.shape
    keep_own = jnp.full((rows, 1), (ids[0] == ids[3]).astype(I32), I32) == 1
    keep_ref[...] = jnp.where(keep_own, own, other)
    send = jnp.where(keep_own, other, own)
    power = power_of(jnp.max(jnp.abs(send), axis=0, keepdims=True))
    code_ref[:rows, :] = jnp.round(send * (jnp.exp2(-power) * CODE_TOP)).astype(I32).astype(I16)
    code_ref[rows:, :] = jnp.broadcast_to(power, (TAIL, width)).astype(I32).astype(I16)


def split_near_kernel(own_ref, other_ref, keep_ref, code_ref):
    split_rows(own_ref[...], other_ref[...], keep_ref, code_ref)


def output_last_kernel(tail_d, w_ref, own_block, other_block, own_ref, other_ref, keep_ref, code_ref):
    rows, width = own_block.shape
    groups = w_ref.shape[0] // width
    base = pl.multiple_of(lax.rem(ids[2] + groups - tail_d, groups) * width, width)
    left = jnp.concatenate([own_block[...], other_block[...]], axis=0)
    part = jnp.dot(left, w_ref[pl.ds(base, width), :], preferred_element_type=F32)
    split_rows(own_ref[...] + part[:rows], other_ref[...] + part[rows:], keep_ref, code_ref)


def finish_kernel(keep_near, got_near, keep_far, got_far, text_ref, out_ref):
    half = out_ref.shape[0]
    rows = half // 2
    for far, (keep_ref, got_ref) in enumerate(((keep_near, got_near), (keep_far, got_far))):
        at = pl.multiple_of((ids[1] ^ far) * rows, rows)
        scale = jnp.exp2(got_ref[rows:, :].astype(I32).astype(F32)[:1]) * (1.0 / CODE_TOP)
        total = keep_ref[...] + got_ref[:rows, :].astype(I32).astype(F32) * scale
        text = text_ref[pl.ds(pl.multiple_of(ids[3] * half + at, rows), rows), :]
        out_ref[pl.ds(at, rows), :] = (text.astype(F32) + total).astype(BF16)


def fast_shards(text_states, q_weight, q_gain, key_cache, value_cache, block_mask, lengths, o_weight):
    ctx = lax.axis_size("ctx")
    struct = jax.ShapeDtypeStruct
    text_rows, depth = text_states.shape
    columns = q_weight.shape[1]
    keys = key_cache.shape[0]
    groups = key_cache.shape[1] // LANES
    width = columns // groups
    heads = width // LANES
    rows, half = text_rows // 4, text_rows // 2
    pairs = heads * rows
    segments = block_mask.shape[1]
    out_cols = o_weight.shape[1]

    def swap(value, bits):
        return lax.ppermute(value, "ctx", [(i, i ^ bits) for i in range(ctx)])

    def turn(value, shift):
        return lax.ppermute(value, "ctx", [(i, (i + shift) % ctx) for i in range(ctx)])

    def after(value, *others):
        return lax.optimization_barrier((value, *others))[0]

    in_hbm = functools.partial(pltpu.with_memory_space_constraint, memory_space=pltpu.HBM)
    order = list(range(groups - 1, -1, -1))
    chunks = [groups - 1, *[d for d in range(1, groups - 1)], 0]
    packs = call(
        pack_kernel,
        (struct((2 * keys + TAIL, LANES), BF16),) * groups,
        (in_hbm(key_cache), in_hbm(value_cache), in_hbm(block_mask.T)),
        specs=[HB] * 3,
        scratch=[
            pltpu.VMEM(key_cache.shape, BF16),
            pltpu.VMEM(value_cache.shape, BF16),
            pltpu.VMEM((segments, text_rows), I32),
            pltpu.SemaphoreType.DMA((3,)),
        ],
    )
    source = after(in_hbm(text_states), packs[0])
    packs = [packs[0]] + [swap(packs[d], 4 * d) for d in range(1, groups)]
    sent, kept, sent_more, kept_more = call(
        functools.partial(project_kernel, chunks),
        (*[struct((half, width), F32)] * 2, *[struct((half, (groups - 1) * width), F32)] * 2),
        (source, in_hbm(q_weight)),
        flops=2 * text_rows * depth * columns,
        specs=[HB] * 2,
        scratch=[
            pltpu.VMEM(text_states.shape, BF16),
            pltpu.VMEM((groups, depth, width), BF16),
            pltpu.SemaphoreType.DMA((groups + 1,)),
        ],
    )
    halves = (kept, swap(sent, 1))
    more = (kept_more, swap(sent_more, 1))

    sums = {}
    for n, d in enumerate(chunks):
        code, own = call(
            functools.partial(split_x_kernel, max(n - 1, 0)),
            (struct((pairs + TAIL, LANES), I16), struct((rows, width), F32)),
            more if n else halves,
        )
        got = swap(code, 2)
        (out,) = call(
            functools.partial(split_z_kernel, [d]),
            (struct((pairs + TAIL, LANES), I16) if d else struct((rows, width), F32),),
            (own, got),
        )
        sums[d] = swap(out, 4 * d) if d else out
    normed = call(
        norm_kernel,
        struct((rows, width), BF16),
        (sums[0], q_gain.reshape(1, LANES), *[sums[d] for d in range(1, groups)]),
    )

    lens = lengths.reshape(2, LANES)
    last = groups // 2
    first = [d for d in order[::-1] if d != last]
    queries = {t: swap(normed, t) if t else normed for t in range(4)}
    states, previous = {}, ()
    for rel in range(4):
        states[rel] = call(
            functools.partial(attend_kernel, first, heads, segments, rel, True, False),
            (struct((LANES, pairs), F32), struct((8, pairs), F32)),
            (after(queries[rel], *previous), lens, *[packs[d] for d in first]),
            flops=4 * pairs * keys * len(first) * LANES,
        )
        previous = states[rel]
    outs = {}
    for rel in (2, 3, 1, 0):
        if rel:
            shape = struct((LANES + TAIL, pairs), I16)
        else:
            shape = (struct((LANES, pairs), F32), struct((8, pairs), F32))
        res = call(
            functools.partial(attend_kernel, [last], heads, segments, rel, False, True),
            shape,
            (after(queries[rel], previous), lens, packs[last], *states[rel]),
            flops=4 * pairs * keys * LANES,
        )
        previous = res
        outs[rel] = swap(res, rel) if rel else res
    attended = call(
        functools.partial(merge_kernel, heads), struct((rows, width), BF16), (*outs[0], outs[1], outs[2], outs[3])
    )

    column = {d: turn(attended, 4 * d) if d else attended for d in order}
    beside = {d: swap(column[d], 2) for d in range(groups)}
    early, late = list(range(groups // 2)), list(range(groups // 2, groups))
    tail_d = late[0]

    def over_core(values):
        if len(values) == 1:
            return [swap(values[0], 1)]
        moved = swap(jnp.stack(values), 1)
        return [moved[i] for i in range(len(values))]

    blocks = {}
    moved = over_core([b for d in early for b in (column[d], beside[d])])
    for i, d in enumerate(early):
        blocks[d] = (column[d], beside[d], moved[2 * i], moved[2 * i + 1])
    pairs_late = [(d, side) for d in reversed(late) for side in (column, beside)][:-1]
    moved = over_core([side[d] for d, side in pairs_late])
    end = over_core([beside[tail_d]])
    moved = moved + end
    for i, d in enumerate(reversed(late)):
        blocks[d] = (column[d], beside[d], moved[2 * i], moved[2 * i + 1])
    piece = struct((rows, out_cols), F32)
    done = (piece, struct((rows + TAIL, out_cols), I16))

    def output_rows(side):
        parts = [b for d in order for b in blocks[d][2 * side : 2 * side + (1 if d == tail_d else 2)]]
        return call(
            functools.partial(output_rows_kernel, order, tail_d),
            (piece, piece),
            (o_weight, *parts),
            flops=4 * rows * columns * out_cols,
        )

    def trade(code):
        return lax.ppermute(code, ("head", "tp"), [(0, 1), (1, 0)])

    near_own, far_own = output_rows(0)
    near_other, far_other = output_rows(1)
    keep_near, code = call(split_near_kernel, done, (near_own, near_other))
    got_near = trade(code)
    keep_far, code = call(
        functools.partial(output_last_kernel, tail_d),
        done,
        (o_weight, blocks[tail_d][1], blocks[tail_d][3], far_own, far_other),
        flops=4 * rows * width * out_cols,
    )
    got_far = trade(code)
    return call(finish_kernel, struct((half, out_cols), BF16), (keep_near, got_near, keep_far, got_far, text_states))


def plain_shards(
    text_states,
    q_weight,
    q_gain,
    visual_key_cache,
    visual_value_cache,
    block_mask,
    lengths,
    o_weight,
):
    text_rows = text_states.shape[0]
    columns = q_weight.shape[1]
    head_dim = q_gain.shape[0]
    query_heads = columns // head_dim
    kv_heads = visual_key_cache.shape[1] // head_dim
    query_group_count = query_heads // kv_heads
    row_block = text_states
    query_share = lax.psum_scatter(
        jnp.dot(row_block, q_weight, preferred_element_type=jnp.float32),
        "ctx",
        scatter_dimension=0,
        tiled=True,
    )
    shaped = query_share.reshape(query_share.shape[0], query_heads, head_dim)
    mean_sq = jnp.mean(shaped * shaped, axis=-1, keepdims=True)
    normed = shaped * lax.rsqrt(mean_sq + 1e-05) * q_gain
    queries = lax.all_gather(
        normed.reshape(query_share.shape[0], columns).astype(jnp.bfloat16),
        "ctx",
        axis=0,
        tiled=True,
    )
    keys_local = visual_key_cache.shape[0]
    segment_len = keys_local // block_mask.shape[1]
    key_block_offset = lax.axis_index("ctx") * keys_local
    positions = key_block_offset + jnp.arange(keys_local, dtype=jnp.int32)
    allowed = (jnp.repeat(block_mask, segment_len, axis=1) == 1) & (
        positions[None, :] < lengths[:, None]
    )
    score_scale = 1.0 / head_dim**0.5
    partial_nums = []
    partial_maxes = []
    partial_totals = []
    for q_head in range(query_heads):
        kv_head = q_head // query_group_count
        query_part = queries[:, q_head * head_dim : (q_head + 1) * head_dim]
        key_part = visual_key_cache[:, kv_head * head_dim : (kv_head + 1) * head_dim]
        value_part = visual_value_cache[:, kv_head * head_dim : (kv_head + 1) * head_dim]
        scores = (
            lax.dot_general(
                query_part, key_part, (((1,), (1,)), ((), ())), preferred_element_type=jnp.float32
            )
            * score_scale
        )
        scores = jnp.where(allowed, scores, jnp.float32(-1e30))
        local_max = jnp.max(scores, axis=1)
        weights = jnp.where(allowed, jnp.exp(scores - local_max[:, None]), jnp.float32(0.0))
        partial_totals.append(jnp.sum(weights, axis=1))
        partial_maxes.append(local_max)
        partial_nums.append(
            jnp.dot(weights.astype(jnp.bfloat16), value_part, preferred_element_type=jnp.float32)
        )
    local_num = jnp.concatenate(partial_nums, axis=1)
    local_max = jnp.stack(partial_maxes, axis=1)
    local_total = jnp.stack(partial_totals, axis=1)
    highest = lax.pmax(local_max, "ctx")
    factor = jnp.exp(local_max - highest)
    scaled_num = local_num * jnp.repeat(factor, head_dim, axis=1)
    scaled_total = local_total * factor
    owned_num, owned_total = (
        lax.psum_scatter(scaled_num, "ctx", scatter_dimension=0, tiled=True),
        lax.psum_scatter(scaled_total, "ctx", scatter_dimension=0, tiled=True),
    )
    owned = (owned_num / jnp.repeat(owned_total, head_dim, axis=1)).astype(jnp.bfloat16)
    attended = lax.all_gather(owned, "ctx", axis=0, tiled=True)
    rows_out = text_rows // lax.axis_size(("head", "tp"))
    row_block = attended
    summed = lax.psum_scatter(
        jnp.dot(row_block, o_weight, preferred_element_type=jnp.float32),
        ("head", "tp"),
        scatter_dimension=0,
        tiled=True,
    )
    residual = lax.dynamic_slice_in_dim(
        text_states, lax.axis_index(("head", "tp")) * rows_out, rows_out, 0
    )
    return (residual.astype(jnp.float32) + summed).astype(jnp.bfloat16)


def solution(mesh):
    in_specs = (
        P(None, "ctx"),
        P("ctx", ("head", "tp")),
        P(),
        P("ctx", ("head", "tp")),
        P("ctx", ("head", "tp")),
        P(None, "ctx"),
        P(),
        P(("head", "tp"), "ctx"),
    )
    out_specs = P(("head", "tp"), "ctx")
    ctx, halves = mesh.shape["ctx"], mesh.shape["head"] * mesh.shape["tp"]

    def fits(args):
        text_rows = args[0].shape[0]
        groups = args[3].shape[1] // args[2].shape[0]
        return (
            args[2].shape[0] == LANES
            and halves == 2
            and text_rows == 2 * LANES
            and groups == 4
            and ctx == 4 * groups
            and args[1].shape[1] % (groups * LANES) == 0
            and args[1].shape[1] // groups <= LANES * LANES
            and 2 * args[5].shape[1] <= TAIL
            and args[3].shape[0] % (args[5].shape[1] * LANES) == 0
        )

    def shards(*args):
        if not fits(args):
            return plain_shards(*args)
        return fast_shards(*args)

    spread = jax.shard_map(shards, mesh=mesh, in_specs=in_specs, out_specs=out_specs, check_vma=False)
    if halves != 2 or ctx != 16:
        return spread
    return spread
```
